32 devices in a mesh: groups: 2 (over y), seq: 4 (over x, core), qset: 4 (over z).
Axes of the slice: x: 2, y: 2, z: 4, core: 2. Of those that a mesh axis runs over, the one named last changes fastest.
Arguments:
- states: bfloat16 [8, 4, 128, 4096], P(('groups', 'qset'), 'seq'), parts along dimension 0, may hold values from -7 to 7
- enc_gain: bfloat16 [4096], replicated, may hold values from 0.25 to 1.75
- dec_states: bfloat16 [16, 64, 4096], P(('groups', 'qset')), parts along dimension 0, may hold values from -7 to 7
- dec_gain: bfloat16 [4096], replicated, may hold values from 0.25 to 1.75
- query_weight: bfloat16 [4096, 4096], P(None, 'seq'), may hold values from -0.375 to 0.375
- key_value_weight: bfloat16 [4096, 2, 4096], P(None, None, 'seq'), may hold values from -0.0625 to 0.0625
- out_weight: bfloat16 [4096, 4096], P('seq'), may hold values from -0.75 to 0.75
- question_of: int32 [8, 4, 1], P('groups'), parts along dimension 0, may hold values from 0 to 7; in each aligned block of 4 rows (0 to 3, 4 to 7, ..., all dimensions but the last counted through in order) at most 2 rows name the same one
Outputs:
- mixed: bfloat16 [16, 64, 4096], P(('groups', 'qset'), None, 'seq'), parts along dimension 0
The draws below stay inside these ranges and needn't reach their ends.
There are 2 independent parts, one for each index of `groups`. The reference program is written for one: setup_inputs(seed, part) draws one part's arguments, and reference() takes and returns one part's arrays. A program takes and returns all parts, laid end to end along the dimension named above; an argument that names none is the same for every part. Nothing has to cross between parts.
Inputs may be any that keep to these rules, and one draw needn't show every extreme that they name: `question_of`: within each index of the first dimension (one source group of 4 passages) at most 2 passages name the same question, and exactly 2 do for some question in some groups; every question is named by at least one passage.
All inputs are finite; a program needn't handle non-finite values.
Results may differ from the reference program's by a relative error of at most 0.014.
The reference program's roundings to bfloat16 on the way count: a program that leaves them out, or rounds other values in their place, can miss the bound.
Values may be sent and summed in bfloat16 or wider, within the bound.
A program may use at most 128 MiB of HBM per device.

```python
import math
import jax
import jax.numpy as jnp
import numpy as np
from jax import lax

D = 4096
HEADS = 64
HD = 64
PLEN = 128
CAP = 2
DTOK = 64
QUESTIONS = 8
N_SEQ = 4
N_QSET = 4


def drawn_rows(salt_key, lead_shape):
    values = jax.random.normal(jax.random.fold_in(salt_key, 105), lead_shape + (D,), jnp.float32)
    return jnp.clip(values, -6.0, 6.0)


def draw_states(key, part):
    salt_key = jax.random.fold_in(key, 11)
    lead_shape = (N_QSET, N_SEQ, PLEN)
    result = drawn_rows(salt_key, lead_shape)
    return result.astype(jnp.bfloat16)


def draw_dec_states(key, part):
    salt_key = jax.random.fold_in(key, 12)
    lead_shape = (QUESTIONS, DTOK)
    result = drawn_rows(salt_key, lead_shape)
    return result.astype(jnp.bfloat16)


def weight_tables(key):
    key_part = jax.random.normal(jax.random.fold_in(key, 201), (D, 2, HEADS * HD), jnp.float32)
    key_part = jnp.clip(key_part, -4.0, 4.0) * D ** (-0.5)
    query_part = jax.random.normal(jax.random.fold_in(key, 202), (D, HEADS * HD), jnp.float32)
    query_part = jnp.clip(query_part, -4.0, 4.0) * (D * HD) ** (-0.5)
    return (key_part, query_part)


def draw_key_value_weight(key, part):
    key_part, query_part = weight_tables(key)
    return key_part.astype(jnp.bfloat16)


def draw_query_weight(key, part):
    key_part, query_part = weight_tables(key)
    result = query_part
    return result.astype(jnp.bfloat16)


def steps_of(own_key, dims, split, low, largest):
    def one(dim, blocks):
        draws = jax.random.uniform(jax.random.fold_in(jax.random.fold_in(own_key, 6), dim), (blocks,), jnp.float32, low / len(split), largest / len(split))
        return jnp.repeat(jnp.exp(draws), dims[dim] // blocks).reshape((-1,) + (1,) * (len(dims) - dim - 1))

    loudness = one(*split[0])
    for cut in split[1:]:
        loudness = loudness * one(*cut)
    return loudness


def shared_out(rng, own, number, rows, amount, top, bound, slope):
    order = jax.random.permutation(rng, amount)
    heavy_load, ordinary = load_shares(amount, rows * top, bound, slope, True), load_shares(amount, rows * top, bound, slope, False)
    places = jnp.arange(amount)

    def named(tallies, offset_by):
        used = int((tallies > 0).sum())
        fixed = max(1, used // 4)
        shifted = fixed + (places - fixed + offset_by * (used - fixed)) % max(1, amount - fixed)
        return jnp.zeros((amount,), jnp.int32).at[order[jnp.where(places < fixed, places, shifted)]].set(jnp.asarray(tallies, jnp.int32))

    tallies = jnp.where(number % 4 == 0, named(heavy_load, number // 4), named(ordinary, number - number // 4 - 1))
    mixed = jax.random.permutation(jax.random.fold_in(own, 3), amount)
    giver, sink = mixed[0:amount // 2 * 2:2], mixed[1:amount // 2 * 2:2]
    room = jnp.minimum(tallies[giver] - 1, bound - tallies[sink]) // 2
    room = jnp.where((giver == order[0]) | (sink == order[0]) | (tallies[sink] == 0), 0, jnp.maximum(room, 0))
    shifted = jax.random.randint(jax.random.fold_in(own, 4), (amount // 2,), 0, 1 << 20) % (room + 1)
    tallies = tallies.at[giver].add(-shifted).at[sink].add(shifted)
    items = jnp.searchsorted(jnp.cumsum(tallies), jnp.arange(rows * top), side="right").astype(jnp.int32)
    table = items.reshape(top, rows).T
    table = table[jax.random.permutation(jax.random.fold_in(own, 1), rows)]
    offset_by = jax.random.randint(jax.random.fold_in(own, 2), (rows, 1), 0, top)
    return jnp.take_along_axis(table, (jnp.arange(top)[None, :] + offset_by) % top, axis=1)


def load_shares(amount, total, reach, skew, full):
    portions = [(1 << 20) // math.isqrt(rank ** skew) + 1 for rank in range(1, amount + 1)]
    largest = reach if full else min(reach, max(-(-total // amount), total * portions[0] // sum(portions)))
    least = 1 if total - largest >= amount - 1 else 0
    given, surplus = [largest] + [least] * (amount - 1), total - largest - least * (amount - 1)
    while surplus > 0:
        movable = [i for i in range(1, amount) if given[i] < largest] or [i for i in range(1, amount) if given[i] < reach]
        whole, budget = sum([portions[i] for i in movable]), surplus
        for i in movable:
            more = min(reach - given[i], max(1, budget * portions[i] // whole), surplus)
            given[i] = given[i] + more
            surplus = surplus - more
    return np.array(given)


def normal_values(rng, shape, width, limit, split=(), held_as=jnp.bfloat16):
    array = jax.random.normal(rng, shape, jnp.float32) * width
    if len(split) > 0:
        array = steps_of(rng, shape, split, -0.22, 0.18) * array
    return jnp.clip(array, min=-limit, max=limit).astype(held_as)


def setup_inputs(seed: int = 0, part: int = 0) -> dict:
    arg_keys = jax.random.split(jax.random.key(seed), 9)
    part_keys = jax.random.split(jax.random.fold_in(arg_keys[8], part), 9)
    states = draw_states(jax.random.fold_in(jax.random.fold_in(arg_keys[8], part), 71), part)
    enc_gain = jnp.clip(1.0 + 0.15 * jax.random.normal(arg_keys[1], (D,), jnp.float32), 0.25, 1.75).astype(jnp.bfloat16)
    dec_states = draw_dec_states(jax.random.fold_in(jax.random.fold_in(arg_keys[8], part), 71), part)
    dec_gain = jnp.clip(1.0 + 0.15 * jax.random.normal(arg_keys[3], (D,), jnp.float32), 0.25, 1.75).astype(jnp.bfloat16)
    query_weight = draw_query_weight(jax.random.fold_in(arg_keys[8], 71), part)
    key_value_weight = draw_key_value_weight(jax.random.fold_in(arg_keys[8], 71), part)
    out_weight = normal_values(arg_keys[6], (HEADS * HD, D), HD ** -0.5, 0.75, ((0, 4),))
    question_of_keys = jax.random.split(jax.random.fold_in(part_keys[7], 1), N_QSET * N_SEQ // N_SEQ)
    question_of_turns = jax.random.permutation(jax.random.fold_in(part_keys[7], 3), N_QSET * N_SEQ // N_SEQ)
    question_of = jax.vmap(lambda own, number: shared_out(jax.random.fold_in(part_keys[7], 2), own, number, N_SEQ, QUESTIONS, 1, CAP, 2))(question_of_keys, question_of_turns).reshape((N_QSET, N_SEQ, 1))
    return {"states": states, "enc_gain": enc_gain, "dec_states": dec_states, "dec_gain": dec_gain, "query_weight": query_weight, "key_value_weight": key_value_weight, "out_weight": out_weight, "question_of": question_of}


EPSILON = 1e-06
MASKED_SCORE = -1e+30

def scaled_norm(rows_in, gain_vec):
    rows_f32 = rows_in.astype(jnp.float32)
    mean_square = lax.optimization_barrier(jnp.mean(rows_f32 * rows_f32, axis=-1, keepdims=True))
    return rows_f32 * lax.rsqrt(mean_square + EPSILON) * gain_vec.astype(jnp.float32)

def rounded(values_in):
    return lax.optimization_barrier(values_in.astype(jnp.bfloat16)).astype(jnp.float32)

def reference(states, enc_gain, dec_states, dec_gain, query_weight, key_value_weight, out_weight, question_of):
    enc_rows = scaled_norm(states, enc_gain).astype(jnp.bfloat16).reshape(-1, D)
    passage_question = question_of.reshape(-1).astype(jnp.int32)
    row_question = jnp.repeat(passage_question, PLEN)
    question_count = dec_states.shape[0]
    live_mask = row_question[None, :] == jnp.arange(question_count, dtype=jnp.int32)[:, None]
    dec_rows = scaled_norm(dec_states, dec_gain).astype(jnp.bfloat16).reshape(-1, D)
    query_heads = jnp.transpose(query_weight.reshape(D, HEADS, HD), (1, 0, 2))
    key_heads = jnp.transpose(key_value_weight[:, 0, :].reshape(D, HEADS, HD), (1, 0, 2))
    value_heads = jnp.transpose(key_value_weight[:, 1, :].reshape(D, HEADS, HD), (1, 0, 2))
    out_heads = out_weight.reshape(HEADS, HD, D)

    def one_head(carry, weights_in):
        w_query, w_key, w_value, w_out = weights_in
        queries = jnp.dot(dec_rows, w_query, preferred_element_type=jnp.float32).astype(jnp.bfloat16)
        key_rows = jnp.dot(enc_rows, w_key, preferred_element_type=jnp.float32).astype(jnp.bfloat16)
        value_rows = jnp.dot(enc_rows, w_value, preferred_element_type=jnp.float32).astype(jnp.bfloat16)
        query_blocks = rounded(queries).reshape(question_count, -1, HD)
        scores = jnp.einsum('qtd,rd->qtr', query_blocks, key_rows.astype(jnp.float32))
        scores = jnp.where(live_mask[:, None, :], scores, MASKED_SCORE)
        row_peak = lax.optimization_barrier(jnp.max(scores, axis=-1, keepdims=True))
        weights = jnp.where(live_mask[:, None, :], jnp.exp(scores - row_peak), 0.0)
        row_total = lax.optimization_barrier(jnp.sum(weights, axis=-1, keepdims=True))
        summed = jnp.einsum('qtr,rd->qtd', rounded(weights), value_rows.astype(jnp.float32))
        attended = (summed / row_total).astype(jnp.bfloat16).reshape(-1, HD)
        return (carry + jnp.dot(attended, w_out, preferred_element_type=jnp.float32), None)
    start_sum = jnp.zeros((dec_rows.shape[0], D), jnp.float32)
    projected, unused = lax.scan(one_head, start_sum, (query_heads, key_heads, value_heads, out_heads))
    mixed = dec_states.astype(jnp.float32) + projected.reshape(dec_states.shape)
    return mixed.astype(jnp.bfloat16)
```

```python
import functools
import jax
import jax.numpy as jnp
from jax import lax
from jax.experimental import pallas as pl
from jax.experimental.pallas import tpu as pltpu
from jax.sharding import PartitionSpec as P

HD = 64
EPSILON = 1e-06
DEAD = -1e30
CH = 2
F32 = jnp.float32
BF16 = jnp.bfloat16
scope = jax.named_scope


def norm_rows(load, store, gain, rows):
    step = 16

    def one(i, carry):
        at = pl.multiple_of(i * step, step)
        x = load(at, step).astype(F32)
        ms = jnp.mean(x * x, axis=-1, keepdims=True)
        store(at, step, (x * lax.rsqrt(ms + EPSILON) * gain).astype(BF16))
        return carry

    lax.fori_loop(0, rows // step, one, 0, unroll=2)


def kernel(
    cfg, qo, states, enc_gain, dec_states, dec_gain, qw, kvw, ow, out,
    xin, dec_v, gat, qw_v, raw, pulled, kv_v, ow_v, xn, kvs, qall, a_s, e_s,
    ps, es, pr, er, att, dsend, dpart, xsend, rx, rown,
    local_sem, raw_sem, ow_sem, xp_send, xs_send, xf_send, xs_recv, q_send, q_recv,
    ps_send, es_send, pr_recv, er_recv, d_send, d_recv, r_send, r_recv,
):
    n_seq, nz, nlq, plen, dlen, width, cols = cfg
    nx = n_seq // 2
    npairs = cols // 128
    rows = nlq * dlen
    hr = plen // 2
    cr = hr // CH
    piece = width // n_seq
    me = lax.axis_index("seq")
    z = lax.axis_index("qset")
    x = me // 2
    c = lax.rem(me, 2)
    partner = x * 2 + (1 - c)
    up_ok = z < nz - 1
    down_ok = z > 0

    def seq_of(dx, core):
        return lax.rem(x + dx, nx) * 2 + core

    barrier = pltpu.get_barrier_semaphore()
    for dx in range(1, nx):
        pl.semaphore_signal(barrier, 1, device_id={"seq": seq_of(dx, c)})
    pl.semaphore_signal(barrier, 1, device_id={"seq": partner})

    @pl.when(up_ok)
    def _():
        pl.semaphore_signal(barrier, 1, device_id={"qset": z + 1})

    @pl.when(down_ok)
    def _():
        pl.semaphore_signal(barrier, 1, device_id={"qset": z - 1})

    own_copy = pltpu.make_async_copy(states, xin, local_sem.at[0])
    own_copy.start()
    dec_copy = pltpu.make_async_copy(dec_states, dec_v, local_sem.at[1])
    dec_copy.start()
    qw_copy = pltpu.make_async_copy(qw, qw_v, local_sem.at[2])
    qw_copy.start()
    nblocks = cols // 128
    slots = raw.shape[0]
    kv2 = kvw.reshape(2 * width, cols)

    def raw_copy(b):
        return pltpu.make_async_copy(
            kv2.at[:, pl.ds(b * 128, 128)], raw.at[b % slots], raw_sem.at[b % slots]
        )

    def ow_copy(b):
        i, h2, k = b // 4, (b // 2) % 2, b % 2
        src = (2 * i + k) * 128 + h2 * HD
        return pltpu.make_async_copy(
            ow.at[pl.ds(src, HD)], ow_v.at[pl.ds(b * HD, HD)], ow_sem.at[b]
        )

    eg = enc_gain[...].astype(F32).reshape(1, width)
    dg = dec_gain[...].astype(F32).reshape(1, width)
    own_copy.wait()
    for b in range(min(slots, nblocks)):
        raw_copy(b).start()

    def put_own(at, n, v):
        gat[me, pl.ds(at, n), :] = v

    with scope("own_norm"):
        norm_rows(lambda at, n: xin[pl.ds(at, n), :], put_own, eg, plen)
    with scope("barrier"):
        pl.semaphore_wait(
            barrier, nx - 1 + 1 + up_ok.astype(jnp.int32) + down_ok.astype(jnp.int32)
        )

    def state_copy(slot, half, ch, to, send_sem):
        part = gat.at[slot, pl.ds(pl.multiple_of(half * hr + ch * cr, cr), cr)]
        return pltpu.make_async_remote_copy(
            src_ref=part, dst_ref=part, send_sem=send_sem,
            recv_sem=xs_recv.at[slot, half * CH + ch], device_id={"seq": to},
        )

    def wait_state(slot, half, ch):
        state_copy(slot, half, ch, partner, xp_send.at[0, 0]).wait_recv()

    def to_partner(first, ch):
        half = 1 - c if first else c
        return state_copy(me, half, ch, partner, xp_send.at[0 if first else 1, ch])

    def over_x(k, dx, ch):
        return state_copy(x * 2 + k, c, ch, seq_of(dx, c), xs_send.at[k, dx, ch])

    def start_over_x(k):
        for ch in range(CH):
            for dx in range(1, nx):
                over_x(k, dx, ch).start()

    def passed_on(k, dx, ch):
        return state_copy(seq_of(dx, k), c, ch, partner, xf_send.at[k, dx, ch])

    def forward(k, ch):
        for dx in range(1, nx):
            wait_state(seq_of(dx, k), c, ch)
            passed_on(k, dx, ch).start()

    for ch in range(CH):
        to_partner(True, ch).start()

    @pl.when(c == 0)
    def _():
        start_over_x(0)

    for ch in range(CH):
        to_partner(False, ch).start()

    def put_xn(at, n, v):
        xn[pl.ds(at, n), :] = v

    with scope("dec_norm"):
        dec_copy.wait()
        norm_rows(lambda at, n: dec_v[pl.ds(at, n), :], put_xn, dg, rows)

    with scope("x_start"):
        for ch in range(CH):
            wait_state(partner, c, ch)

        @pl.when(c == 1)
        def _():
            start_over_x(0)

        start_over_x(1)

    def q_copy(up, question):
        part = qall.at[question]
        return pltpu.make_async_remote_copy(
            src_ref=part, dst_ref=part, send_sem=q_send.at[0 if up else 1, question],
            recv_sem=q_recv.at[question], device_id={"qset": z + 1 if up else z - 1},
        )

    tile = min(256, cols)
    with scope("qproj"):
        qw_copy.wait()

        def q_tile(i, carry):
            at = pl.ds(pl.multiple_of(i * tile, tile), tile)
            r = jnp.dot(xn[...], qw_v[:, at], preferred_element_type=F32).astype(BF16)
            for lq in range(nlq):
                qall[z * nlq + lq, :, at] = r[lq * dlen:(lq + 1) * dlen]
            return carry

        lax.fori_loop(0, cols // tile, q_tile, 0, unroll=2)
    for lq in range(nlq):
        @pl.when(up_ok)
        def _():
            q_copy(True, z * nlq + lq).start()

        @pl.when(down_ok)
        def _():
            q_copy(False, z * nlq + lq).start()

    def pass_q(j, lq):
        @pl.when((z - j >= 0) & up_ok)
        def _():
            q_copy(True, (z - j) * nlq + lq).wait_recv()
            q_copy(True, (z - j) * nlq + lq).start()

        @pl.when((z + j < nz) & down_ok)
        def _():
            q_copy(False, (z + j) * nlq + lq).wait_recv()
            q_copy(False, (z + j) * nlq + lq).start()

    step = 256

    def pull_block(b):
        raw_copy(b).wait()
        flat = raw.at[b % slots]

        def pull(i, carry):
            for u in range(4):
                s = i * 4 + u
                buf = pulled.at[pl.ds(u * step, step)]
                buf[...] = flat[pl.ds(pl.multiple_of(s * step, step), step), :].astype(F32)
                at = pl.ds(pl.multiple_of(s * (step // 2), step // 2), step // 2)
                kv_v[at, pl.ds(b * 128, 128)] = buf[pl.ds(0, step // 2, stride=2), :].astype(BF16)
                kv_v[at, pl.ds(cols + b * 128, 128)] = (
                    buf[pl.ds(1, step // 2, stride=2), :].astype(BF16)
                )
            return carry

        lax.fori_loop(0, 2 * width // step // 4, pull, 0)
        if b + slots < nblocks:
            raw_copy(b + slots).start()

    with scope("pull"):
        for b in range(nblocks):
            pull_block(b)
            if b == (nblocks + 1) // 2 and nz > 2:
                pass_q(1, 0)
    for b in range(cols // HD):
        ow_copy(b).start()

    flat_gat = gat.reshape(n_seq * plen, width)
    flat_kvs = kvs.reshape(n_seq * plen, 2 * cols)
    ktile = min(256, cols)

    def project(first, count, lo, hi):
        base = pl.multiple_of(first * plen, plen)

        def kv_tile(i, carry):
            at = pl.ds(pl.multiple_of(i * ktile, ktile), ktile)
            r = jnp.dot(
                flat_gat[pl.ds(base, count * plen), :], kv_v[:, at],
                preferred_element_type=F32,
            )
            flat_kvs[pl.ds(base, count * plen), at] = r.astype(BF16)
            return carry

        lax.fori_loop(lo * cols // ktile, hi * cols // ktile, kv_tile, 0, unroll=2)

    with scope("fwd0"):
        forward(0, 0)
    with scope("q_fwd0"):
        if nz > 2:
            for lq in range(1, nlq):
                pass_q(1, lq)
        for ch in range(CH):
            wait_state(partner, 1 - c, ch)
    with scope("proj_own0"):
        project(x * 2, 2, 0, 1)
    with scope("q_fwd1"):
        if nz > 3:
            pass_q(2, 0)
    with scope("proj_own1"):
        project(x * 2, 2, 1, 2)
    with scope("fwd1"):
        if nz > 3:
            for lq in range(1, nlq):
                pass_q(2, lq)
        forward(0, 1)
        for ch in range(CH):
            for dx in range(1, nx):
                wait_state(seq_of(dx, 0), 1 - c, ch)
    with scope("proj_a"):
        for dx in range(1, nx):
            project(seq_of(dx, 0), 1, 0, 2)
    with scope("q_fwd2"):
        for j in range(3, nz - 1):
            for lq in range(nlq):
                pass_q(j, lq)
    with scope("fwd2"):
        forward(1, 0)

    low = lax.broadcasted_iota(jnp.int32, (dlen, 128), 1) < HD

    def attend(p, j):
        at = pl.ds(pl.multiple_of(j * 128, 128), 128)
        vat = pl.ds(pl.multiple_of(cols + j * 128, 128), 128)
        q = qall[qo[z, p], :, at]
        zero = jnp.zeros_like(q)
        q2 = jnp.concatenate([jnp.where(low, q, zero), jnp.where(low, zero, q)], axis=0)
        s = lax.dot_general(
            kvs[p, :, at], q2, (((1,), (1,)), ((), ())), preferred_element_type=F32
        )
        m = jnp.max(s, axis=0, keepdims=True)
        w = jnp.exp(s - m)
        l = jnp.sum(w, axis=0, keepdims=True)
        o = lax.dot_general(
            kvs[p, :, vat], w.astype(BF16), (((0,), (0,)), ((), ())),
            preferred_element_type=F32,
        )
        a = jnp.where(low, o[:HD], o[HD:]) * (1.0 / l)
        a_s[p, pl.ds(pl.multiple_of(j * HD, HD), HD), :] = a
        e_s[p, pl.ds(j, 1), :] = m + jnp.log(l)

    def attend_all(ps_list):
        for p in ps_list:
            lax.fori_loop(0, npairs, lambda j, carry, p=p: (attend(p, j), carry)[1], 0, unroll=8 if npairs % 8 == 0 else 1)

    if npairs < 8:
        e_s[...] = jnp.zeros(e_s.shape, F32)
    with scope("wait_q"):
        for question in range(nlq * nz):
            b = question // nlq

            @pl.when(((b < z) & (z == nz - 1)) | ((b > z) & (z == 0)))
            def _():
                q_copy(True, question).wait_recv()
    with scope("attend_own"):
        attend_all([x * 2, x * 2 + 1])
    with scope("attend_a"):
        attend_all([seq_of(dx, 0) for dx in range(1, nx)])

    @pl.when(z == 0)
    def _():
        er[0] = jnp.full(er.shape[1:], DEAD, F32)
        pr[0] = jnp.zeros(pr.shape[1:], BF16)

    @pl.when(z == nz - 1)
    def _():
        er[1] = jnp.full(er.shape[1:], DEAD, F32)
        pr[1] = jnp.zeros(pr.shape[1:], BF16)

    with scope("fwd3"):
        forward(1, 1)
        for ch in range(CH):
            for dx in range(1, nx):
                wait_state(seq_of(dx, 1), 1 - c, ch)
    with scope("proj_b"):
        for dx in range(1, nx):
            project(seq_of(dx, 1), 1, 0, 2)
    with scope("attend_b"):
        attend_all([seq_of(dx, 1) for dx in range(1, nx)])

    def terms(question, others):
        first = jnp.int32(0)
        second = jnp.int32(0)
        count = jnp.int32(0)
        for p in range(n_seq):
            hit = qo[z, p] == question
            first = jnp.where(hit & (count == 0), p, first)
            second = jnp.where(hit & (count == 1), p, second)
            count = count + hit.astype(jnp.int32)
        e = [jnp.where(count >= 1, e_s[first], DEAD), jnp.where(count >= 2, e_s[second], DEAD)]
        e += [er[d, question] for d in others]
        top = functools.reduce(jnp.maximum, e)
        w = [jnp.exp(t - top) for t in e]
        tot = functools.reduce(jnp.add, w)
        inv = 1.0 / tot
        w = [t * inv for t in w]

        def block(j):
            at = pl.ds(j * HD, HD)
            parts = [a_s[first, at, :], a_s[second, at, :]]
            parts += [pr[d, question, at, :].astype(F32) for d in others]
            return functools.reduce(
                jnp.add, [t * u[j:j + 1, :] for t, u in zip(parts, w, strict=True)]
            )

        return block, top + jnp.log(tot)

    def result_copies(d, question):
        to = z + 1 - 2 * d
        return [
            pltpu.make_async_remote_copy(
                src_ref=src.at[d, question], dst_ref=dst.at[d, question],
                send_sem=ss.at[d, question], recv_sem=rs.at[d, question],
                device_id={"qset": to},
            )
            for src, dst, ss, rs in ((es, er, es_send, er_recv), (ps, pr, ps_send, pr_recv))
        ]

    def sends(d, dest):
        return jnp.where(d == 0, dest > z, dest < z)

    def hop(d, k, lq):
        dest = jnp.where(d == 0, nz - 1 - k, k)
        question = dest * nlq + lq

        @pl.when(sends(d, dest))
        def _():
            @pl.when(jnp.where(d == 0, z > 0, z < nz - 1))
            def _():
                for cp in result_copies(d, question):
                    cp.wait_recv()

            block, e = terms(question, [d])
            for j in range(npairs):
                ps[d, question, pl.ds(j * HD, HD), :] = block(j).astype(BF16)
            es[d, question] = e
            for cp in result_copies(d, question):
                cp.start()

    near = (2 * z >= nz).astype(jnp.int32)
    with scope("chain"):
        for k in range(nz - 1):
            for d in (near, 1 - near):
                for lq in range(nlq):
                    hop(d, k, lq)

    ptile = min(512, piece)
    order = list(range(1, nx)) + [0]

    def project_out(lq, dest, put):
        for i in range(piece // ptile):
            src = pl.ds(pl.multiple_of(dest * piece + i * ptile, 128), ptile)
            put(pl.ds(i * ptile, ptile), jnp.dot(att[lq], ow_v[:, src], preferred_element_type=F32))

    def d_copy(lq, dx):
        return pltpu.make_async_remote_copy(
            src_ref=dsend.at[lq, dx], dst_ref=dpart.at[lq, dx], send_sem=d_send.at[lq, dx],
            recv_sem=d_recv.at[lq, dx], device_id={"seq": partner},
        )

    def r_copy(lq, dx):
        return pltpu.make_async_remote_copy(
            src_ref=xsend.at[lq, dx], dst_ref=rx.at[lq, x], send_sem=r_send.at[lq, dx],
            recv_sem=r_recv.at[lq, x], device_id={"seq": seq_of(dx, c)},
        )

    for lq in range(nlq):
        question = z * nlq + lq
        with scope("wait_res"):
            for d in range(2):
                @pl.when(z > 0 if d == 0 else z < nz - 1)
                def _():
                    for cp in result_copies(d, question):
                        cp.wait_recv()
        with scope("finish"):
            block, _ = terms(question, [0, 1])
            for i in range(npairs // 2):
                t = jnp.transpose(jnp.concatenate([block(2 * i), block(2 * i + 1)], axis=0))
                t = t.astype(BF16)
                att[lq, :, pl.ds(2 * i * 128, 128)] = t[:HD]
                att[lq, :, pl.ds((2 * i + 1) * 128, 128)] = t[HD:]
            if lq == 0:
                for b in range(cols // HD):
                    ow_copy(b).wait()
        with scope("out"):
            for dx in order:
                def put_send(at, r):
                    dsend[lq, dx, :, at] = r.astype(BF16)

                project_out(lq, seq_of(dx, 1 - c), put_send)
                d_copy(lq, dx).start()
            for dx in order:
                def put_sum(at, r):
                    rown[lq, dx, :, at] = r

                project_out(lq, seq_of(dx, c), put_sum)
        with scope("pair_sum"):
            for dx in order:
                d_copy(lq, dx).wait_recv()
                both = rown[lq, dx] + dpart[lq, dx].astype(F32)
                if dx:
                    xsend[lq, dx] = both.astype(BF16)
                    r_copy(lq, dx).start()
                else:
                    mine = pl.ds(pl.multiple_of(me * piece, 128), piece)
                    rown[lq, 0] = both + dec_v[pl.ds(lq * dlen, dlen), mine].astype(F32)
    for lq in range(nlq):
        with scope("final"):
            total = rown[lq, 0]
            for dx in range(1, nx):
                xs = lax.rem(x + dx, nx)
                pltpu.make_async_remote_copy(
                    src_ref=xsend.at[lq, 0], dst_ref=rx.at[lq, xs], send_sem=r_send.at[lq, 0],
                    recv_sem=r_recv.at[lq, xs], device_id={"seq": xs * 2 + c},
                ).wait_recv()
                total = total + rx[lq, xs].astype(F32)
            out[pl.ds(lq * dlen, dlen), :] = total.astype(BF16)

    for ch in range(CH):
        to_partner(True, ch).wait_send()
        to_partner(False, ch).wait_send()
        for k in range(2):
            for dx in range(1, nx):
                over_x(k, dx, ch).wait_send()
                passed_on(k, dx, ch).wait_send()
    for question in range(nlq * nz):
        b = question // nlq

        @pl.when(up_ok & (b <= z))
        def _():
            q_copy(True, question).wait_send()

        @pl.when(down_ok & (b >= z))
        def _():
            q_copy(False, question).wait_send()

        for d in range(2):
            @pl.when(sends(d, b))
            def _():
                for cp in result_copies(d, question):
                    cp.wait_send()
    for lq in range(nlq):
        for dx in range(nx):
            d_copy(lq, dx).wait_send()
            if dx:
                r_copy(lq, dx).wait_send()


def body(
    states, enc_gain, dec_states, dec_gain, query_weight, key_value_weight, out_weight, question_of
):
    nz = lax.axis_size("qset")
    n_seq = lax.axis_size("seq")
    nx = n_seq // 2
    plen, width = states.shape[2], states.shape[3]
    nlq, dlen = dec_states.shape[0], dec_states.shape[1]
    cols = query_weight.shape[1]
    rows = nlq * dlen
    piece = width // n_seq
    half = cols // 2
    nq = nlq * nz
    slots = min(4, cols // 128)
    cfg = (n_seq, nz, nlq, plen, dlen, width, cols)
    any_spec = pl.BlockSpec(memory_space=pl.ANY)
    vmem = pl.BlockSpec(memory_space=pltpu.VMEM)
    dma = pltpu.SemaphoreType.DMA
    result = pl.pallas_call(
        functools.partial(kernel, cfg),
        out_shape=jax.ShapeDtypeStruct((rows, piece), BF16),
        in_specs=[pl.BlockSpec(memory_space=pltpu.SMEM), any_spec, vmem, any_spec, vmem,
                  any_spec, any_spec, any_spec],
        out_specs=vmem,
        scratch_shapes=[
            pltpu.VMEM((plen, width), BF16),
            pltpu.VMEM((rows, width), BF16),
            pltpu.VMEM((n_seq, plen, width), BF16),
            pltpu.VMEM((width, cols), BF16),
            pltpu.VMEM((slots, 2 * width, 128), BF16),
            pltpu.VMEM((1024, 128), F32),
            pltpu.VMEM((width, 2 * cols), BF16),
            pltpu.VMEM((cols, width), BF16),
            pltpu.VMEM((rows, width), BF16),
            pltpu.VMEM((n_seq, plen, 2 * cols), BF16),
            pltpu.VMEM((nq, dlen, cols), BF16),
            pltpu.VMEM((n_seq, half, 128), F32),
            pltpu.VMEM((n_seq, 8, 128), F32),
            pltpu.VMEM((2, nq, half, 128), BF16),
            pltpu.VMEM((2, nq, 8, 128), F32),
            pltpu.VMEM((2, nq, half, 128), BF16),
            pltpu.VMEM((2, nq, 8, 128), F32),
            pltpu.VMEM((nlq, dlen, cols), BF16),
            pltpu.VMEM((nlq, nx, dlen, piece), BF16),
            pltpu.VMEM((nlq, nx, dlen, piece), BF16),
            pltpu.VMEM((nlq, nx, dlen, piece), BF16),
            pltpu.VMEM((nlq, nx, dlen, piece), BF16),
            pltpu.VMEM((nlq, nx, dlen, piece), F32),
            dma((3,)), dma((slots,)), dma((cols // HD,)),
            dma((2, CH)), dma((2, nx, CH)), dma((2, nx, CH)), dma((n_seq, 2 * CH)),
            dma((2, nq)), dma((nq,)),
            dma((2, nq)), dma((2, nq)), dma((2, nq)), dma((2, nq)),
            dma((nlq, nx)), dma((nlq, nx)), dma((nlq, nx)), dma((nlq, nx)),
        ],
        compiler_params=pltpu.CompilerParams(
            collective_id=0, has_side_effects=True, vmem_limit_bytes=63 * 1024 * 1024
        ),
        name="reader",
    )(
        question_of[:, :, 0], states.reshape(plen, width), enc_gain,
        dec_states.reshape(rows, width), dec_gain,
        query_weight, key_value_weight, out_weight,
    )
    return result.reshape(nlq, dlen, piece)


def solution(mesh):
    return jax.shard_map(
        body,
        mesh=mesh,
        in_specs=(
            P(("groups", "qset"), "seq", None, None),
            P(),
            P(("groups", "qset"), None, None),
            P(),
            P(None, "seq"),
            P(None, None, "seq"),
            P("seq", None),
            P("groups", None, None),
        ),
        out_specs=P(("groups", "qset"), None, "seq"),
        check_vma=False,
    )
```

```python
import functools
import jax
import jax.numpy as jnp
from jax import lax
from jax.experimental import pallas as pl
from jax.experimental.pallas import tpu as pltpu
from jax.sharding import PartitionSpec as P

HD = 64
EPSILON = 1e-06
DEAD = -1e30
CHUNKS = (2, 4)
KT = 1024
F32 = jnp.float32
BF16 = jnp.bfloat16
scope = jax.named_scope


def norm_rows(load, store, gain, rows):
    step = 16

    def one(i, carry):
        at = pl.multiple_of(i * step, step)
        x = load(at, step).astype(F32)
        ms = jnp.mean(x * x, axis=-1, keepdims=True)
        store(at, step, (x * lax.rsqrt(ms + EPSILON) * gain).astype(BF16))
        return carry

    lax.fori_loop(0, rows // step, one, 0, unroll=2)


def kernel(
    cfg, qo, states, enc_gain, dec_states, dec_gain, qw, kvw, ow, out,
    eg_v, dg_v, xin, dec_v, gat, qw_v, raw, pulled, kv_v, ow_v, xn, kvs, qall, a_s, e_s,
    ps, pr, pick, att, dsend, dpart, xsend, rx, rown, s_buf, w_buf, i_buf, out_v, acc, pacc,
    local_sem, raw_sem, ow_sem, xp_send, xp_recv, xs_send, xf_send, x_recv, q_send, q_recv,
    ps_send, pr_recv, d_send, d_recv, r_send, r_recv, out_sem,
):
    n_seq, nz, nlq, plen, dlen, width, cols = cfg
    nx = n_seq // 2
    npairs = cols // 128
    rows = nlq * dlen
    hr = plen // 2
    srows = cols // 2
    parts = 2 if npairs % 4 == 0 else 1
    prows = srows // parts
    ppairs = npairs // parts
    beyond = nlq * (nz - 1)
    packed = min(n_seq, beyond)
    piece = width // n_seq
    me = lax.axis_index("seq")
    z = lax.axis_index("qset")
    x = me // 2
    c = lax.rem(me, 2)
    partner = x * 2 + (1 - c)
    up_ok = z < nz - 1
    down_ok = z > 0

    def seq_of(dx, core):
        return lax.rem(x + dx, nx) * 2 + core

    barrier = pltpu.get_barrier_semaphore()
    for dx in range(1, nx):
        pl.semaphore_signal(barrier, 1, device_id={"seq": seq_of(dx, c)})
    pl.semaphore_signal(barrier, 1, device_id={"seq": partner})

    @pl.when(up_ok)
    def _():
        pl.semaphore_signal(barrier, 1, device_id={"qset": z + 1})

    @pl.when(down_ok)
    def _():
        pl.semaphore_signal(barrier, 1, device_id={"qset": z - 1})

    eg_copy = pltpu.make_async_copy(enc_gain, eg_v, local_sem.at[0])
    eg_copy.start()

    def own_copy(half):
        at = pl.ds(half * hr, hr)
        return pltpu.make_async_copy(states.at[at], xin.at[at], local_sem.at[1 + half])

    own_copy(0).start()
    own_copy(1).start()
    dg_copy = pltpu.make_async_copy(dec_gain, dg_v, local_sem.at[3])
    dg_copy.start()
    dec_copy = pltpu.make_async_copy(dec_states, dec_v, local_sem.at[4])
    dec_copy.start()
    qw_copy = pltpu.make_async_copy(qw, qw_v, local_sem.at[5])
    qw_copy.start()
    nblocks = cols // 128
    slots = raw.shape[0]
    kv2 = kvw.reshape(2 * width, cols)

    def raw_copy(b):
        return pltpu.make_async_copy(
            kv2.at[:, pl.ds(b * 128, 128)], raw.at[b % slots], raw_sem.at[b % slots]
        )

    def ow_copy(b):
        i, h2, k = b // 4, (b // 2) % 2, b % 2
        src = (2 * i + k) * 128 + h2 * HD
        return pltpu.make_async_copy(
            ow.at[pl.ds(src, HD)], ow_v.at[pl.ds(b * HD, HD)], ow_sem.at[0]
        )

    eg_copy.wait()
    eg = eg_v[...].astype(F32).reshape(1, width)

    def norm_own(half):
        own_copy(half).wait()

        def put(at, n, v):
            gat[me, pl.ds(half * hr + at, n), :] = v

        norm_rows(lambda at, n: xin[pl.ds(half * hr + at, n), :], put, eg, hr)

    with scope("own_norm"):
        norm_own(0)
    for b in range(min(slots, nblocks)):
        raw_copy(b).start()
    with scope("barrier"):
        pl.semaphore_wait(
            barrier, nx - 1 + 1 + up_ok.astype(jnp.int32) + down_ok.astype(jnp.int32)
        )

    def half_rows(slot, half):
        return gat.at[slot, pl.ds(pl.multiple_of(half * hr, hr), hr)]

    def to_partner(half):
        part = half_rows(me, half)
        return pltpu.make_async_remote_copy(
            src_ref=part, dst_ref=part, send_sem=xp_send.at[half], recv_sem=xp_recv.at[half],
            device_id={"seq": partner},
        )

    def from_partner(half):
        part = half_rows(partner, half)
        return pltpu.make_async_remote_copy(
            src_ref=part, dst_ref=part, send_sem=xp_send.at[half], recv_sem=xp_recv.at[half],
            device_id={"seq": partner},
        )

    def x_copy(slot, half, k, ch, to, send_sem, source):
        wide = width // CHUNKS[k]
        part = gat.at[
            slot, pl.ds(pl.multiple_of(half * hr, hr), hr), pl.ds(ch * wide, wide)
        ]
        return pltpu.make_async_remote_copy(
            src_ref=part, dst_ref=part, send_sem=send_sem,
            recv_sem=x_recv.at[source, half, k * CHUNKS[0] + ch], device_id={"seq": to},
        )

    def over_x(k, dx, ch):
        return x_copy(
            x * 2 + k, c, k, ch, seq_of(dx, c), xs_send.at[dx - 1, k * CHUNKS[0] + ch],
            nx - 1 - dx,
        )

    def start_over_x(k):
        for ch in range(CHUNKS[k]):
            for dx in range(1, nx):
                over_x(k, dx, ch).start()

    def passed_on(k, dx, ch, half):
        return x_copy(
            seq_of(dx, k), half, k, ch, partner, xf_send.at[dx - 1, k * CHUNKS[0] + ch], dx - 1
        )

    def forward(k, ch):
        for dx in range(1, nx):
            passed_on(k, dx, ch, c).wait_recv()
            passed_on(k, dx, ch, c).start()

    def wait_other(k, ch):
        for dx in range(1, nx):
            passed_on(k, dx, ch, 1 - c).wait_recv()

    @pl.when(c == 0)
    def _():
        start_over_x(0)

    @pl.when(c == 1)
    def _():
        to_partner(0).start()

    with scope("own_norm"):
        norm_own(1)
    to_partner(1).start()

    @pl.when(c == 0)
    def _():
        to_partner(0).start()

    def put_xn(at, n, v):
        xn[pl.ds(at, n), :] = v

    with scope("dec_norm"):
        dg_copy.wait()
        dec_copy.wait()
        dg = dg_v[...].astype(F32).reshape(1, width)
        norm_rows(lambda at, n: dec_v[pl.ds(at, n), :], put_xn, dg, rows)

    with scope("x_start"):
        from_partner(c).wait_recv()

        @pl.when(c == 1)
        def _():
            start_over_x(0)

        start_over_x(1)

    def q_copy(up, question):
        part = qall.at[question]
        return pltpu.make_async_remote_copy(
            src_ref=part, dst_ref=part, send_sem=q_send.at[0 if up else 1, question],
            recv_sem=q_recv.at[question], device_id={"qset": z + 1 if up else z - 1},
        )

    tile = min(512, cols)
    with scope("qproj"):
        qw_copy.wait()

        def q_tile(i, carry):
            at = pl.ds(pl.multiple_of(i * tile, tile), tile)
            r = jnp.dot(xn[...], qw_v[:, at], preferred_element_type=F32).astype(BF16)
            for lq in range(nlq):
                qall[z * nlq + lq, :, at] = r[lq * dlen:(lq + 1) * dlen]
            return carry

        lax.fori_loop(0, cols // tile, q_tile, 0)
    for lq in range(nlq):
        @pl.when(up_ok)
        def _():
            q_copy(True, z * nlq + lq).start()

        @pl.when(down_ok)
        def _():
            q_copy(False, z * nlq + lq).start()

    def pass_q(j, lq):
        @pl.when((z - j >= 0) & up_ok)
        def _():
            q_copy(True, (z - j) * nlq + lq).wait_recv()
            q_copy(True, (z - j) * nlq + lq).start()

        @pl.when((z + j < nz) & down_ok)
        def _():
            q_copy(False, (z + j) * nlq + lq).wait_recv()
            q_copy(False, (z + j) * nlq + lq).start()

    step = 256

    def pull_block(b):
        raw_copy(b).wait()
        flat = raw.at[b % slots]

        def pull(i, carry):
            for u in range(4):
                s = i * 4 + u
                buf = pulled.at[pl.ds(u * step, step)]
                buf[...] = flat[pl.ds(pl.multiple_of(s * step, step), step), :].astype(F32)
                at = pl.ds(pl.multiple_of(s * (step // 2), step // 2), step // 2)
                kv_v[at, pl.ds(b * 128, 128)] = buf[pl.ds(0, step // 2, stride=2), :].astype(BF16)
                kv_v[at, pl.ds(cols + b * 128, 128)] = (
                    buf[pl.ds(1, step // 2, stride=2), :].astype(BF16)
                )
            return carry

        lax.fori_loop(0, 2 * width // step // 4, pull, 0)
        if b + slots < nblocks:
            raw_copy(b + slots).start()

    with scope("pull"):
        for b in range(nblocks):
            pull_block(b)
            if b == (nblocks + 1) // 2 and nz > 2:
                pass_q(1, 0)
    for b in range(cols // HD):
        ow_copy(b).start()

    flat_gat = gat.reshape(n_seq * plen, width)
    flat_kvs = kvs.reshape(n_seq * plen, 2 * cols)


    def project(first, count, lo, hi):
        base = pl.multiple_of(first * plen, plen)
        ktile = min(KT // count, cols)

        def kv_tile(i, carry):
            at = pl.ds(pl.multiple_of(i * ktile, ktile), ktile)
            r = jnp.dot(
                flat_gat[pl.ds(base, count * plen), :], kv_v[:, at],
                preferred_element_type=F32,
            )
            flat_kvs[pl.ds(base, count * plen), at] = r.astype(BF16)
            return carry

        lax.fori_loop(lo * cols // ktile, hi * cols // ktile, kv_tile, 0)

    with scope("fwd0"):
        forward(0, 0)
    with scope("q_fwd0"):
        if nz > 2:
            for lq in range(1, nlq):
                pass_q(1, lq)
        from_partner(1 - c).wait_recv()
    with scope("proj_own0"):
        project(x * 2, 2, 0, 1)
    with scope("q_fwd1"):
        if nz > 3:
            pass_q(2, 0)
    with scope("proj_own1"):
        project(x * 2, 2, 1, 2)
    with scope("fwd1"):
        if nz > 3:
            for lq in range(1, nlq):
                pass_q(2, lq)
        for ch in range(1, CHUNKS[0]):
            forward(0, ch)
        for ch in range(CHUNKS[0]):
            wait_other(0, ch)
    with scope("proj_a"):
        for dx in range(1, nx):
            project(seq_of(dx, 0), 1, 0, 2)
    with scope("q_fwd2"):
        for j in range(3, nz - 1):
            for lq in range(nlq):
                pass_q(j, lq)
    wide = width // CHUNKS[1]

    def project_part(dx, ch):
        p = seq_of(dx, 1)
        tile = min(KT, cols)
        for i in range(2 * cols // tile):
            at = pl.ds(i * tile, tile)
            r = jnp.dot(
                gat[p, :, pl.ds(ch * wide, wide)], kv_v[pl.ds(ch * wide, wide), at],
                preferred_element_type=F32,
            )
            if ch:
                r = r + acc[dx - 1, :, at]
            if ch < CHUNKS[1] - 1:
                acc[dx - 1, :, at] = r
            else:
                kvs[p, :, at] = r.astype(BF16)

    def take_part(ch):
        wait_other(1, ch)
        for dx in range(1, nx):
            project_part(dx, ch)

    with scope("b01"):
        forward(1, 0)
        forward(1, 1)
        take_part(0)
        take_part(1)
    with scope("b2"):
        forward(1, 2)
        take_part(2)

    low = lax.broadcasted_iota(jnp.int32, (dlen, 128), 1) < HD

    def attend_all(ps_list):
        units = [(u * npairs + j, p, j) for u, p in enumerate(ps_list) for j in range(npairs)]
        for n, p, j in units:
            q = qall[qo[z, p], :, pl.ds(j * 128, 128)]
            zero = jnp.zeros_like(q)
            q2 = jnp.concatenate([jnp.where(low, q, zero), jnp.where(low, zero, q)], axis=0)
            s_buf[n] = lax.dot_general(
                kvs[p, :, pl.ds(j * 128, 128)], q2, (((1,), (1,)), ((), ())),
                preferred_element_type=F32,
            )
        for n, p, j in units:
            s = s_buf[n]
            m = jnp.max(s, axis=0, keepdims=True)
            w = jnp.exp(s - m)
            l = jnp.sum(w, axis=0, keepdims=True)
            w_buf[n] = w.astype(BF16)
            i_buf[pl.ds(n, 1), :] = 1.0 / l
            e_s[p, pl.ds(j, 1), :] = m + jnp.log(l)
        for n, p, j in units:
            o = lax.dot_general(
                kvs[p, :, pl.ds(cols + j * 128, 128)], w_buf[n], (((0,), (0,)), ((), ())),
                preferred_element_type=F32,
            )
            a_s[p, pl.ds(j * HD, HD), :] = jnp.where(low, o[:HD], o[HD:]) * i_buf[n:n + 1, :]

    if npairs < 8:
        e_s[...] = jnp.zeros(e_s.shape, F32)
    with scope("wait_q"):
        for question in range(nlq * nz):
            b = question // nlq

            @pl.when(((b < z) & (z == nz - 1)) | ((b > z) & (z == 0)))
            def _():
                q_copy(True, question).wait_recv()
    with scope("fwd3"):
        forward(1, 3)
    with scope("attend_own"):
        attend_all([x * 2, x * 2 + 1])
    with scope("attend_a"):
        for dx in range(1, nx):
            attend_all([seq_of(dx, 0)])

    def put_logs(ref, e):
        hi = e.astype(BF16)
        rest = e - hi.astype(F32)
        mid = rest.astype(BF16)
        lo = (rest - mid.astype(F32)).astype(BF16)
        ref[pl.ds(prows, 16), :] = jnp.concatenate([hi, mid], axis=0)
        ref[pl.ds(prows + 16, 16), :] = jnp.concatenate([lo, jnp.zeros_like(lo)], axis=0)

    def get_logs(ref):
        two = ref[pl.ds(prows, 16), :].astype(F32)
        return two[:8] + two[8:] + ref[pl.ds(prows + 16, 16), :].astype(F32)[:8]

    with scope("b3"):
        take_part(3)
    with scope("attend_b"):
        for dx in range(1, nx):
            attend_all([seq_of(dx, 1)])

    near = (2 * z >= nz).astype(jnp.int32)
    sides = (near, 1 - near)

    def question_at(d, o):
        return jnp.where(d == 0, (nz - 1 - o // nlq) * nlq, o // nlq * nlq) + o % nlq

    def packing(d):
        edge = jnp.where(d == 0, 0, nz - 1)
        rank, ranks, found = jnp.int32(0), [], []
        for o in range(beyond):
            hit = jnp.int32(0)
            for p in range(n_seq):
                hit = hit | (qo[edge, p] == question_at(d, o)).astype(jnp.int32)
            ranks.append(jnp.minimum(rank, packed - 1))
            found.append(hit)
            rank = rank + hit
        return ranks, found

    plans = [packing(d) for d in sides]

    def terms(question, sources):
        first = jnp.int32(0)
        second = jnp.int32(0)
        count = jnp.int32(0)
        for p in range(n_seq):
            hit = qo[z, p] == question
            first = jnp.where(hit & (count == 0), p, first)
            second = jnp.where(hit & (count == 1), p, second)
            count = count + hit.astype(jnp.int32)
        e = [jnp.where(count >= 1, e_s[first], DEAD), jnp.where(count >= 2, e_s[second], DEAD)]
        e += [jnp.where(ok, get_logs(pick.at[side]), DEAD) for side, ok in sources]
        top = functools.reduce(jnp.maximum, e)
        w = [jnp.exp(t - top) for t in e]
        tot = functools.reduce(jnp.add, w)
        inv = 1.0 / tot
        w = [t * inv for t in w]

        def block(j):
            at = pl.ds(j * HD, HD)
            there = pl.ds(j * HD + (32 if j >= ppairs else 0), HD)
            values = [a_s[first, at, :], a_s[second, at, :]]
            values += [pick[side, there, :].astype(F32) for side, ok in sources]
            return functools.reduce(
                jnp.add, [t * u[j:j + 1, :] for t, u in zip(values, w, strict=True)]
            )

        return block, top + jnp.log(tot)

    def part_rows(h):
        return pl.ds(0, prows + 32) if h == 0 else pl.ds(prows + 32, prows)

    def result_copy(d, n, h):
        at = part_rows(h)
        return pltpu.make_async_remote_copy(
            src_ref=ps.at[d, n, at], dst_ref=pr.at[d, n, at], send_sem=ps_send.at[d, n, h],
            recv_sem=pr_recv.at[d, n, h], device_id={"qset": z + 1 - 2 * d},
        )

    def at_edge(d):
        return jnp.where(d == 0, z == 0, z == nz - 1)

    def after_edge(d):
        return jnp.where(d == 0, z == 1, z == nz - 2)

    def places(d):
        return jnp.where(d == 0, nz - 1 - z, z) * nlq

    def take(side, o, packed_o, h):
        d = sides[side]
        at = part_rows(h)
        ranks, _ = plans[side]

        @pl.when(after_edge(d))
        def _():
            if packed_o < packed:
                result_copy(d, packed_o, h).wait_recv()
            value = pr[d, 0, at, :]
            for n in range(1, min(packed_o, packed - 1) + 1):
                value = jnp.where(ranks[packed_o] == n, pr[d, n, at, :], value)
            pick[side, at, :] = value

        @pl.when(~(after_edge(d) | at_edge(d)))
        def _():
            result_copy(d, o, h).wait_recv()
            pick[side, at, :] = pr[d, o, at, :]

        @pl.when(at_edge(d))
        def _():
            pick[side, at, :] = jnp.zeros((at.size, 128), BF16)

    def have(side, packed_o):
        d = sides[side]
        _, found = plans[side]
        return ~at_edge(d) & (~after_edge(d) | (found[packed_o] > 0))

    def put_slot(d, n, block, e, h):
        for j in range(h * ppairs, (h + 1) * ppairs):
            ps[d, n, pl.ds(j * HD + (32 if h else 0), HD), :] = block(j).astype(BF16)
        if h == 0:
            put_logs(ps.at[d, n], e)
        result_copy(d, n, h).start()

    def first_hop(side):
        d = sides[side]
        ranks, found = plans[side]

        @pl.when(at_edge(d))
        def _():
            for n in range(packed):
                question = jnp.int32(-1)
                rank = jnp.int32(0)
                for o in range(beyond):
                    question = jnp.where((found[o] > 0) & (rank == n), question_at(d, o), question)
                    rank = rank + found[o]
                block, e = terms(question, [])
                for h in range(parts):
                    put_slot(d, n, block, e, h)

    def hop(side, o):
        d = sides[side]

        @pl.when((o < places(d)) & ~at_edge(d))
        def _():
            take(side, o, o, 0)
            block, e = terms(question_at(d, o), [(side, have(side, o))])
            put_slot(d, o, block, e, 0)
            for h in range(1, parts):
                take(side, o, o, h)
                put_slot(d, o, block, e, h)

    for question in range(nlq * nz):
        @pl.when(up_ok & (question // nlq <= z))
        def _():
            q_copy(True, question).wait_send()

        @pl.when(down_ok & (question // nlq >= z))
        def _():
            q_copy(False, question).wait_send()

    with scope("chain"):
        for side in range(2):
            first_hop(side)
        for k in range(nz - 1):
            for side in range(2):
                for lq in range(nlq):
                    hop(side, k * nlq + lq)

    for half in range(2):
        to_partner(half).wait_send()
    for k in range(2):
        for ch in range(CHUNKS[k]):
            for dx in range(1, nx):
                over_x(k, dx, ch).wait_send()
                passed_on(k, dx, ch, c).wait_send()

    order = list(range(1, nx)) + [0]

    def product(lq, dest, h):
        src = pl.ds(pl.multiple_of(dest * piece, piece), piece)
        heads = pl.ds(h * ppairs * 128, ppairs * 128)
        return jnp.dot(att[lq, :, heads], ow_v[heads, src], preferred_element_type=F32)

    def d_copy(lq, dx):
        return pltpu.make_async_remote_copy(
            src_ref=dsend.at[lq, dx], dst_ref=dpart.at[lq, dx], send_sem=d_send.at[lq, dx],
            recv_sem=d_recv.at[lq, dx], device_id={"seq": partner},
        )

    def r_copy(lq, dx):
        return pltpu.make_async_remote_copy(
            src_ref=xsend.at[lq, dx], dst_ref=rx.at[lq, x], send_sem=r_send.at[lq, dx - 1],
            recv_sem=r_recv.at[lq, nx - 1 - dx], device_id={"seq": seq_of(dx, c)},
        )

    for lq in range(nlq):
        def own_parts(h):
            with scope("wait_res"):
                last = beyond - nlq + lq
                for side in range(2):
                    take(side, places(sides[side]) + lq, last, h)
            with scope("finish"):
                block, _ = terms(z * nlq + lq, [(side, have(side, last)) for side in range(2)])
                for i in range(h * ppairs // 2, (h + 1) * ppairs // 2):
                    t = jnp.transpose(jnp.concatenate([block(2 * i), block(2 * i + 1)], axis=0))
                    t = t.astype(BF16)
                    att[lq, :, pl.ds(2 * i * 128, 128)] = t[:HD]
                    att[lq, :, pl.ds((2 * i + 1) * 128, 128)] = t[HD:]
                if lq == 0 and h == 0:
                    pltpu.make_async_copy(ow, ow_v, ow_sem.at[0]).wait()

        for h in range(parts - 1):
            own_parts(h)
            with scope("out_part"):
                for n in range(n_seq):
                    dest = seq_of(n // 2, (1 - c) if n % 2 == 0 else c)
                    pacc[n] = product(lq, dest, h)
        own_parts(parts - 1)

        def pair_sum(dx):
            d_copy(lq, dx).wait_recv()
            both = rown[lq, dx] + dpart[lq, dx].astype(F32)
            if dx:
                xsend[lq, dx] = both.astype(BF16)
                r_copy(lq, dx).start()
            else:
                mine = pl.ds(pl.multiple_of(me * piece, 128), piece)
                rown[lq, 0] = both + dec_v[pl.ds(lq * dlen, dlen), mine].astype(F32)

        with scope("out"):
            held = None
            for n, dx in enumerate(order):
                theirs = product(lq, seq_of(dx, 1 - c), parts - 1)
                if parts > 1:
                    theirs = theirs + pacc[2 * dx]
                if held is not None:
                    rown[lq, order[n - 1]] = held
                held = product(lq, seq_of(dx, c), parts - 1)
                if parts > 1:
                    held = held + pacc[2 * dx + 1]
                dsend[lq, dx] = theirs.astype(BF16)
                d_copy(lq, dx).start()
                if n > 1:
                    pair_sum(order[n - 2])
            rown[lq, order[-1]] = held
        with scope("pair_sum"):
            for dx in order[-2:]:
                pair_sum(dx)
    def out_copy(lq):
        return pltpu.make_async_copy(
            out_v.at[lq], out.at[pl.ds(lq * dlen, dlen)], out_sem.at[lq]
        )

    for d in range(2):
        for o in range(beyond):
            sent = (o < places(d)) & ((o < packed) | ~at_edge(d))

            @pl.when(sent)
            def _():
                for h in range(parts):
                    result_copy(d, o, h).wait_send()
    for lq in range(nlq):
        for dx in range(nx):
            d_copy(lq, dx).wait_send()
    for lq in range(nlq):
        with scope("final"):
            total = rown[lq, 0]
            for dx in range(1, nx):
                xs = lax.rem(x + dx, nx)
                pltpu.make_async_remote_copy(
                    src_ref=xsend.at[lq, 0], dst_ref=rx.at[lq, xs], send_sem=r_send.at[lq, 0],
                    recv_sem=r_recv.at[lq, dx - 1], device_id={"seq": xs * 2 + c},
                ).wait_recv()
                total = total + rx[lq, xs].astype(F32)
            out_v[lq] = total.astype(BF16)
            out_copy(lq).start()
    for lq in range(nlq):
        for dx in range(1, nx):
            r_copy(lq, dx).wait_send()
        out_copy(lq).wait()


def body(
    states, enc_gain, dec_states, dec_gain, query_weight, key_value_weight, out_weight, question_of
):
    nz = lax.axis_size("qset")
    n_seq = lax.axis_size("seq")
    nx = n_seq // 2
    plen, width = states.shape[2], states.shape[3]
    nlq, dlen = dec_states.shape[0], dec_states.shape[1]
    cols = query_weight.shape[1]
    rows = nlq * dlen
    piece = width // n_seq
    half = cols // 2
    nq = nlq * nz
    slots = min(3, cols // 128)
    nch = sum(CHUNKS)
    beyond = nlq * (nz - 1)
    parts = 2 if cols % 512 == 0 else 1
    cfg = (n_seq, nz, nlq, plen, dlen, width, cols)
    any_spec = pl.BlockSpec(memory_space=pl.ANY)
    dma = pltpu.SemaphoreType.DMA
    result = pl.pallas_call(
        functools.partial(kernel, cfg),
        out_shape=jax.ShapeDtypeStruct((rows, piece), BF16),
        in_specs=[pl.BlockSpec(memory_space=pltpu.SMEM), any_spec, any_spec, any_spec, any_spec,
                  any_spec, any_spec, any_spec],
        out_specs=any_spec,
        scratch_shapes=[
            pltpu.VMEM((width,), BF16),
            pltpu.VMEM((width,), BF16),
            pltpu.VMEM((plen, width), BF16),
            pltpu.VMEM((rows, width), BF16),
            pltpu.VMEM((n_seq, plen, width), BF16),
            pltpu.VMEM((width, cols), BF16),
            pltpu.VMEM((slots, 2 * width, 128), BF16),
            pltpu.VMEM((1024, 128), F32),
            pltpu.VMEM((width, 2 * cols), BF16),
            pltpu.VMEM((cols, width), BF16),
            pltpu.VMEM((rows, width), BF16),
            pltpu.VMEM((n_seq, plen, 2 * cols), BF16),
            pltpu.VMEM((nq, dlen, cols), BF16),
            pltpu.VMEM((n_seq, half, 128), F32),
            pltpu.VMEM((n_seq, 8, 128), F32),
            pltpu.VMEM((2, beyond, half + 32, 128), BF16),
            pltpu.VMEM((2, beyond, half + 32, 128), BF16),
            pltpu.VMEM((2, half + 32, 128), BF16),
            pltpu.VMEM((nlq, dlen, cols), BF16),
            pltpu.VMEM((nlq, nx, dlen, piece), BF16),
            pltpu.VMEM((nlq, nx, dlen, piece), BF16),
            pltpu.VMEM((nlq, nx, dlen, piece), BF16),
            pltpu.VMEM((nlq, nx, dlen, piece), BF16),
            pltpu.VMEM((nlq, nx, dlen, piece), F32),
            pltpu.VMEM((2 * cols // 128, plen, 128), F32),
            pltpu.VMEM((2 * cols // 128, plen, 128), BF16),
            pltpu.VMEM((max(8, 2 * cols // 128), 128), F32),
            pltpu.VMEM((nlq, dlen, piece), BF16),
            pltpu.VMEM((nx - 1, plen, 2 * cols), F32),
            pltpu.VMEM((n_seq, dlen, piece) if cols % 512 == 0 else (1, 8, 128), F32),
            dma((6,)), dma((slots,)), dma((1,)),
            dma((2,)), dma((2,)), dma((nx - 1, nch)), dma((nx - 1, nch)), dma((nx - 1, 2, nch)),
            dma((2, nq)), dma((nq,)), dma((2, beyond, parts)), dma((2, beyond, parts)),
            dma((nlq, nx)), dma((nlq, nx)), dma((nlq, nx - 1)), dma((nlq, nx - 1)), dma((nlq,)),
        ],
        compiler_params=pltpu.CompilerParams(
            collective_id=0, has_side_effects=True, vmem_limit_bytes=63 * 1024 * 1024
        ),
        name="reader",
    )(
        question_of[:, :, 0], states.reshape(plen, width), enc_gain,
        dec_states.reshape(rows, width), dec_gain,
        query_weight, key_value_weight, out_weight,
    )
    return result.reshape(nlq, dlen, piece)


def solution(mesh):
    return jax.shard_map(
        body,
        mesh=mesh,
        in_specs=(
            P(("groups", "qset"), "seq", None, None),
            P(),
            P(("groups", "qset"), None, None),
            P(),
            P(None, "seq"),
            P(None, None, "seq"),
            P("seq", None),
            P("groups", None, None),
        ),
        out_specs=P(("groups", "qset"), None, "seq"),
        check_vma=False,
    )
```

```python
import functools
import jax
import jax.numpy as jnp
from jax import lax
from jax.experimental import pallas as pl
from jax.experimental.pallas import tpu as pltpu
from jax.sharding import PartitionSpec as P

HD = 64
EPSILON = 1e-06
DEAD = -1e30
CHUNKS = (2, 4)
KT = 1024
F32 = jnp.float32
BF16 = jnp.bfloat16
scope = jax.named_scope


def norm_rows(load, store, gain, rows):
    step = 16

    def one(i, carry):
        at = pl.multiple_of(i * step, step)
        x = load(at, step).astype(F32)
        ms = jnp.mean(x * x, axis=-1, keepdims=True)
        store(at, step, (x * lax.rsqrt(ms + EPSILON) * gain).astype(BF16))
        return carry

    lax.fori_loop(0, rows // step, one, 0, unroll=2)


def kernel(
    cfg, qo, states, enc_gain, dec_states, dec_gain, qw, kvw, ow, out,
    eg_v, dg_v, xin, dec_v, gat, qw_v, raw, pulled, kv_v, ow_v, xn, kvs, qall, a_s, e_s,
    ps, pr, pick, att, dsend, dpart, xsend, rx, rown, s_buf, w_buf, i_buf, acc, pacc,
    local_sem, raw_sem, ow_sem, xp_send, xp_recv, xs_send, xf_send, x_recv, q_send, q_recv,
    ps_send, pr_recv, d_send, d_recv, r_send, r_recv,
):
    n_seq, nz, nlq, plen, dlen, width, cols = cfg
    nx = n_seq // 2
    npairs = cols // 128
    rows = nlq * dlen
    hr = plen // 2
    srows = cols // 2
    parts = 2 if npairs % 4 == 0 else 1
    prows = srows // parts
    ppairs = npairs // parts
    beyond = nlq * (nz - 1)
    packed = min(n_seq, beyond)
    piece = width // n_seq
    me = lax.axis_index("seq")
    z = lax.axis_index("qset")
    x = me // 2
    c = lax.rem(me, 2)
    partner = x * 2 + (1 - c)
    up_ok = z < nz - 1
    down_ok = z > 0

    def seq_of(dx, core):
        return lax.rem(x + dx, nx) * 2 + core

    barrier = pltpu.get_barrier_semaphore()
    for dx in range(1, nx):
        pl.semaphore_signal(barrier, 1, device_id={"seq": seq_of(dx, c)})
    pl.semaphore_signal(barrier, 1, device_id={"seq": partner})

    @pl.when(up_ok)
    def _():
        pl.semaphore_signal(barrier, 1, device_id={"qset": z + 1})

    @pl.when(down_ok)
    def _():
        pl.semaphore_signal(barrier, 1, device_id={"qset": z - 1})

    eg_copy = pltpu.make_async_copy(enc_gain, eg_v, local_sem.at[0])
    eg_copy.start()

    def own_copy(half):
        at = pl.ds(half * hr, hr)
        return pltpu.make_async_copy(states.at[at], xin.at[at], local_sem.at[1 + half])

    own_copy(0).start()
    own_copy(1).start()
    dg_copy = pltpu.make_async_copy(dec_gain, dg_v, local_sem.at[3])
    dg_copy.start()
    dec_copy = pltpu.make_async_copy(dec_states, dec_v, local_sem.at[4])
    dec_copy.start()
    qw_copy = pltpu.make_async_copy(qw, qw_v, local_sem.at[5])
    qw_copy.start()
    nblocks = cols // 128
    slots = raw.shape[0]
    kv2 = kvw.reshape(2 * width, cols)

    def raw_copy(b):
        return pltpu.make_async_copy(
            kv2.at[:, pl.ds(b * 128, 128)], raw.at[b % slots], raw_sem.at[b % slots]
        )

    def ow_copy(b):
        i, h2, k = b // 4, (b // 2) % 2, b % 2
        src = (2 * i + k) * 128 + h2 * HD
        return pltpu.make_async_copy(
            ow.at[pl.ds(src, HD)], ow_v.at[pl.ds(b * HD, HD)], ow_sem.at[0]
        )

    eg_copy.wait()
    eg = eg_v[...].astype(F32).reshape(1, width)

    def norm_own(half):
        own_copy(half).wait()

        def put(at, n, v):
            gat[me, pl.ds(half * hr + at, n), :] = v

        norm_rows(lambda at, n: xin[pl.ds(half * hr + at, n), :], put, eg, hr)

    with scope("own_norm"):
        norm_own(0)
    for b in range(min(slots, nblocks)):
        raw_copy(b).start()
    with scope("barrier"):
        pl.semaphore_wait(
            barrier, nx - 1 + 1 + up_ok.astype(jnp.int32) + down_ok.astype(jnp.int32)
        )

    def half_rows(slot, half):
        return gat.at[slot, pl.ds(pl.multiple_of(half * hr, hr), hr)]

    def to_partner(half):
        part = half_rows(me, half)
        return pltpu.make_async_remote_copy(
            src_ref=part, dst_ref=part, send_sem=xp_send.at[half], recv_sem=xp_recv.at[half],
            device_id={"seq": partner},
        )

    def from_partner(half):
        part = half_rows(partner, half)
        return pltpu.make_async_remote_copy(
            src_ref=part, dst_ref=part, send_sem=xp_send.at[half], recv_sem=xp_recv.at[half],
            device_id={"seq": partner},
        )

    def x_copy(slot, half, k, ch, to, send_sem, source):
        wide = width // CHUNKS[k]
        part = gat.at[
            slot, pl.ds(pl.multiple_of(half * hr, hr), hr), pl.ds(ch * wide, wide)
        ]
        return pltpu.make_async_remote_copy(
            src_ref=part, dst_ref=part, send_sem=send_sem,
            recv_sem=x_recv.at[source, half, k * CHUNKS[0] + ch], device_id={"seq": to},
        )

    def over_x(k, dx, ch):
        return x_copy(
            x * 2 + k, c, k, ch, seq_of(dx, c), xs_send.at[dx - 1, k * CHUNKS[0] + ch],
            nx - 1 - dx,
        )

    def start_over_x(k):
        for ch in range(CHUNKS[k]):
            for dx in range(1, nx):
                over_x(k, dx, ch).start()

    def passed_on(k, dx, ch, half):
        return x_copy(
            seq_of(dx, k), half, k, ch, partner, xf_send.at[dx - 1, k * CHUNKS[0] + ch], dx - 1
        )

    def forward(k, ch):
        for dx in range(1, nx):
            passed_on(k, dx, ch, c).wait_recv()
            passed_on(k, dx, ch, c).start()

    def wait_other(k, ch):
        for dx in range(1, nx):
            passed_on(k, dx, ch, 1 - c).wait_recv()

    @pl.when(c == 0)
    def _():
        start_over_x(0)

    @pl.when(c == 1)
    def _():
        to_partner(0).start()

    with scope("own_norm"):
        norm_own(1)
    to_partner(1).start()

    @pl.when(c == 0)
    def _():
        to_partner(0).start()

    def put_xn(at, n, v):
        xn[pl.ds(at, n), :] = v

    with scope("dec_norm"):
        dg_copy.wait()
        dec_copy.wait()
        dg = dg_v[...].astype(F32).reshape(1, width)
        norm_rows(lambda at, n: dec_v[pl.ds(at, n), :], put_xn, dg, rows)

    with scope("x_start"):
        from_partner(c).wait_recv()

        @pl.when(c == 1)
        def _():
            start_over_x(0)

        start_over_x(1)

    def q_copy(up, question):
        part = qall.at[question]
        return pltpu.make_async_remote_copy(
            src_ref=part, dst_ref=part, send_sem=q_send.at[0 if up else 1, question],
            recv_sem=q_recv.at[question], device_id={"qset": z + 1 if up else z - 1},
        )

    tile = min(512, cols)
    with scope("qproj"):
        qw_copy.wait()

        def q_tile(i, carry):
            at = pl.ds(pl.multiple_of(i * tile, tile), tile)
            r = jnp.dot(xn[...], qw_v[:, at], preferred_element_type=F32).astype(BF16)
            for lq in range(nlq):
                qall[z * nlq + lq, :, at] = r[lq * dlen:(lq + 1) * dlen]
            return carry

        lax.fori_loop(0, cols // tile, q_tile, 0)
    for lq in range(nlq):
        @pl.when(up_ok)
        def _():
            q_copy(True, z * nlq + lq).start()

        @pl.when(down_ok)
        def _():
            q_copy(False, z * nlq + lq).start()

    def pass_q(j, lq):
        @pl.when((z - j >= 0) & up_ok)
        def _():
            q_copy(True, (z - j) * nlq + lq).wait_recv()
            q_copy(True, (z - j) * nlq + lq).start()

        @pl.when((z + j < nz) & down_ok)
        def _():
            q_copy(False, (z + j) * nlq + lq).wait_recv()
            q_copy(False, (z + j) * nlq + lq).start()

    step = 256

    def pull_block(b):
        raw_copy(b).wait()
        flat = raw.at[b % slots]

        def pull(i, carry):
            for u in range(4):
                s = i * 4 + u
                buf = pulled.at[pl.ds(u * step, step)]
                buf[...] = flat[pl.ds(pl.multiple_of(s * step, step), step), :].astype(F32)
                at = pl.ds(pl.multiple_of(s * (step // 2), step // 2), step // 2)
                kv_v[at, pl.ds(b * 128, 128)] = buf[pl.ds(0, step // 2, stride=2), :].astype(BF16)
                kv_v[at, pl.ds(cols + b * 128, 128)] = (
                    buf[pl.ds(1, step // 2, stride=2), :].astype(BF16)
                )
            return carry

        lax.fori_loop(0, 2 * width // step // 4, pull, 0)
        if b + slots < nblocks:
            raw_copy(b + slots).start()

    with scope("pull"):
        for b in range(nblocks):
            pull_block(b)
            if b == (nblocks + 1) // 2 and nz > 2:
                pass_q(1, 0)
    for b in range(cols // HD):
        ow_copy(b).start()

    flat_gat = gat.reshape(n_seq * plen, width)
    flat_kvs = kvs.reshape(n_seq * plen, 2 * cols)


    def project(first, count, lo, hi):
        base = pl.multiple_of(first * plen, plen)
        ktile = min(KT // count, cols)

        def kv_tile(i, carry):
            at = pl.ds(pl.multiple_of(i * ktile, ktile), ktile)
            r = jnp.dot(
                flat_gat[pl.ds(base, count * plen), :], kv_v[:, at],
                preferred_element_type=F32,
            )
            flat_kvs[pl.ds(base, count * plen), at] = r.astype(BF16)
            return carry

        lax.fori_loop(lo * cols // ktile, hi * cols // ktile, kv_tile, 0)

    with scope("fwd0"):
        forward(0, 0)
    with scope("q_fwd0"):
        if nz > 2:
            for lq in range(1, nlq):
                pass_q(1, lq)
        from_partner(1 - c).wait_recv()
    with scope("proj_own0"):
        project(x * 2, 2, 0, 1)
    with scope("q_fwd1"):
        for ch in range(1, CHUNKS[0]):
            forward(0, ch)
        if nz > 3:
            pass_q(2, 0)
    with scope("proj_own1"):
        project(x * 2, 2, 1, 2)
    with scope("fwd1"):
        forward(1, 0)
        if nz > 3:
            for lq in range(1, nlq):
                pass_q(2, lq)
        for ch in range(CHUNKS[0]):
            wait_other(0, ch)
    with scope("proj_a"):
        for dx in range(1, nx):
            project(seq_of(dx, 0), 1, 0, 2)
    with scope("q_fwd2"):
        for j in range(3, nz - 1):
            for lq in range(nlq):
                pass_q(j, lq)
    wide = width // CHUNKS[1]

    def project_part(dx, ch):
        p = seq_of(dx, 1)
        tile = min(KT, cols)
        for i in range(2 * cols // tile):
            at = pl.ds(i * tile, tile)
            r = jnp.dot(
                gat[p, :, pl.ds(ch * wide, wide)], kv_v[pl.ds(ch * wide, wide), at],
                preferred_element_type=F32,
            )
            if ch:
                r = r + acc[dx - 1, :, at]
            if ch < CHUNKS[1] - 1:
                acc[dx - 1, :, at] = r
            else:
                kvs[p, :, at] = r.astype(BF16)

    def take_part(ch):
        wait_other(1, ch)
        for dx in range(1, nx):
            project_part(dx, ch)

    with scope("b01"):
        forward(1, 1)
        take_part(0)
        take_part(1)
    with scope("b2"):
        forward(1, 2)
        take_part(2)
    with scope("fwd3"):
        forward(1, 3)

    low = lax.broadcasted_iota(jnp.int32, (dlen, 128), 1) < HD

    def attend_all(ps_list):
        units = [(u * npairs + j, p, j) for u, p in enumerate(ps_list) for j in range(npairs)]
        for n, p, j in units:
            q = qall[qo[z, p], :, pl.ds(j * 128, 128)]
            zero = jnp.zeros_like(q)
            q2 = jnp.concatenate([jnp.where(low, q, zero), jnp.where(low, zero, q)], axis=0)
            s_buf[n] = lax.dot_general(
                kvs[p, :, pl.ds(j * 128, 128)], q2, (((1,), (1,)), ((), ())),
                preferred_element_type=F32,
            )
        for n, p, j in units:
            s = s_buf[n]
            m = jnp.max(s, axis=0, keepdims=True)
            w = jnp.exp(s - m)
            l = jnp.sum(w, axis=0, keepdims=True)
            w_buf[n] = w.astype(BF16)
            i_buf[pl.ds(n, 1), :] = 1.0 / l
            e_s[p, pl.ds(j, 1), :] = m + jnp.log(l)
        for n, p, j in units:
            o = lax.dot_general(
                kvs[p, :, pl.ds(cols + j * 128, 128)], w_buf[n], (((0,), (0,)), ((), ())),
                preferred_element_type=F32,
            )
            a_s[p, pl.ds(j * HD, HD), :] = jnp.where(low, o[:HD], o[HD:]) * i_buf[n:n + 1, :]

    if npairs < 8:
        e_s[...] = jnp.zeros(e_s.shape, F32)
    with scope("wait_q"):
        for question in range(nlq * nz):
            b = question // nlq

            @pl.when(((b < z) & (z == nz - 1)) | ((b > z) & (z == 0)))
            def _():
                q_copy(True, question).wait_recv()
    with scope("attend_own"):
        attend_all([x * 2, x * 2 + 1])
    with scope("attend_a"):
        for dx in range(1, nx):
            attend_all([seq_of(dx, 0)])

    def put_logs(ref, e):
        hi = e.astype(BF16)
        rest = e - hi.astype(F32)
        mid = rest.astype(BF16)
        lo = (rest - mid.astype(F32)).astype(BF16)
        ref[pl.ds(prows, 16), :] = jnp.concatenate([hi, mid], axis=0)
        ref[pl.ds(prows + 16, 16), :] = jnp.concatenate([lo, jnp.zeros_like(lo)], axis=0)

    def get_logs(ref):
        two = ref[pl.ds(prows, 16), :].astype(F32)
        return two[:8] + two[8:] + ref[pl.ds(prows + 16, 16), :].astype(F32)[:8]

    with scope("b3"):
        take_part(3)
    with scope("attend_b"):
        for dx in range(1, nx):
            attend_all([seq_of(dx, 1)])

    near = (2 * z >= nz).astype(jnp.int32)
    sides = (near, 1 - near)

    def question_at(d, o):
        return jnp.where(d == 0, (nz - 1 - o // nlq) * nlq, o // nlq * nlq) + o % nlq

    def packing(d):
        edge = jnp.where(d == 0, 0, nz - 1)
        rank, ranks, found = jnp.int32(0), [], []
        for o in range(beyond):
            hit = jnp.int32(0)
            for p in range(n_seq):
                hit = hit | (qo[edge, p] == question_at(d, o)).astype(jnp.int32)
            ranks.append(jnp.minimum(rank, packed - 1))
            found.append(hit)
            rank = rank + hit
        return ranks, found

    plans = [packing(d) for d in sides]

    def terms(question, sources):
        first = jnp.int32(0)
        second = jnp.int32(0)
        count = jnp.int32(0)
        for p in range(n_seq):
            hit = qo[z, p] == question
            first = jnp.where(hit & (count == 0), p, first)
            second = jnp.where(hit & (count == 1), p, second)
            count = count + hit.astype(jnp.int32)
        e = [jnp.where(count >= 1, e_s[first], DEAD), jnp.where(count >= 2, e_s[second], DEAD)]
        e += [jnp.where(ok, get_logs(pick.at[side]), DEAD) for side, ok in sources]
        top = functools.reduce(jnp.maximum, e)
        w = [jnp.exp(t - top) for t in e]
        tot = functools.reduce(jnp.add, w)
        inv = 1.0 / tot
        w = [t * inv for t in w]

        def block(j):
            at = pl.ds(j * HD, HD)
            there = pl.ds(j * HD + (32 if j >= ppairs else 0), HD)
            values = [a_s[first, at, :], a_s[second, at, :]]
            values += [pick[side, there, :].astype(F32) for side, ok in sources]
            return functools.reduce(
                jnp.add, [t * u[j:j + 1, :] for t, u in zip(values, w, strict=True)]
            )

        return block, top + jnp.log(tot)

    def part_rows(h):
        return pl.ds(0, prows + 32) if h == 0 else pl.ds(prows + 32, prows)

    def result_copy(d, n, h):
        at = part_rows(h)
        return pltpu.make_async_remote_copy(
            src_ref=ps.at[d, n, at], dst_ref=pr.at[d, n, at], send_sem=ps_send.at[d, n, h],
            recv_sem=pr_recv.at[d, n, h], device_id={"qset": z + 1 - 2 * d},
        )

    def at_edge(d):
        return jnp.where(d == 0, z == 0, z == nz - 1)

    def after_edge(d):
        return jnp.where(d == 0, z == 1, z == nz - 2)

    def places(d):
        return jnp.where(d == 0, nz - 1 - z, z) * nlq

    def take(side, o, packed_o, h):
        d = sides[side]
        at = part_rows(h)
        ranks, _ = plans[side]

        @pl.when(after_edge(d))
        def _():
            if packed_o < packed:
                result_copy(d, packed_o, h).wait_recv()
            value = pr[d, 0, at, :]
            for n in range(1, min(packed_o, packed - 1) + 1):
                value = jnp.where(ranks[packed_o] == n, pr[d, n, at, :], value)
            pick[side, at, :] = value

        @pl.when(~(after_edge(d) | at_edge(d)))
        def _():
            result_copy(d, o, h).wait_recv()
            pick[side, at, :] = pr[d, o, at, :]

        @pl.when(at_edge(d))
        def _():
            pick[side, at, :] = jnp.zeros((at.size, 128), BF16)

    def have(side, packed_o):
        d = sides[side]
        _, found = plans[side]
        return ~at_edge(d) & (~after_edge(d) | (found[packed_o] > 0))

    def put_slot(d, n, block, e, h):
        for j in range(h * ppairs, (h + 1) * ppairs):
            ps[d, n, pl.ds(j * HD + (32 if h else 0), HD), :] = block(j).astype(BF16)
        if h == 0:
            put_logs(ps.at[d, n], e)
        result_copy(d, n, h).start()

    def first_hop(side):
        d = sides[side]
        ranks, found = plans[side]

        @pl.when(at_edge(d))
        def _():
            for n in range(packed):
                question = jnp.int32(-1)
                rank = jnp.int32(0)
                for o in range(beyond):
                    question = jnp.where((found[o] > 0) & (rank == n), question_at(d, o), question)
                    rank = rank + found[o]
                block, e = terms(question, [])
                for h in range(parts):
                    put_slot(d, n, block, e, h)

    def hop(side, o):
        d = sides[side]

        @pl.when((o < places(d)) & ~at_edge(d))
        def _():
            take(side, o, o, 0)
            block, e = terms(question_at(d, o), [(side, have(side, o))])
            put_slot(d, o, block, e, 0)
            for h in range(1, parts):
                take(side, o, o, h)
                put_slot(d, o, block, e, h)

    for question in range(nlq * nz):
        @pl.when(up_ok & (question // nlq <= z))
        def _():
            q_copy(True, question).wait_send()

        @pl.when(down_ok & (question // nlq >= z))
        def _():
            q_copy(False, question).wait_send()

    with scope("chain"):
        for side in range(2):
            first_hop(side)
        for o in range(beyond + 1):
            if o < beyond:
                hop(0, o)
            if o:
                hop(1, o - 1)

    for half in range(2):
        to_partner(half).wait_send()
    for k in range(2):
        for ch in range(CHUNKS[k]):
            for dx in range(1, nx):
                over_x(k, dx, ch).wait_send()
                passed_on(k, dx, ch, c).wait_send()


    def product(lq, dest, first, count):
        src = pl.ds(pl.multiple_of(dest * piece, piece), piece)
        heads = pl.ds(first * ppairs * 128, count * ppairs * 128)
        rows_in = pl.ds(lq * dlen, dlen) if lq is not None else pl.ds(0, rows)
        return jnp.dot(att[rows_in, heads], ow_v[heads, src], preferred_element_type=F32)

    def d_copy(lq, dx):
        return pltpu.make_async_remote_copy(
            src_ref=dsend.at[lq, dx], dst_ref=dpart.at[lq, dx], send_sem=d_send.at[lq, dx],
            recv_sem=d_recv.at[lq, dx], device_id={"seq": partner},
        )

    def r_copy(lq, dx):
        return pltpu.make_async_remote_copy(
            src_ref=xsend.at[lq, dx], dst_ref=rx.at[lq, x], send_sem=r_send.at[lq, dx - 1],
            recv_sem=r_recv.at[lq, nx - 1 - dx], device_id={"seq": seq_of(dx, c)},
        )

    def pair_sum(lq, dx):
        d_copy(lq, dx).wait_recv()
        both = rown[lq, dx] + dpart[lq, dx].astype(F32)
        if dx:
            xsend[lq, dx] = both.astype(BF16)
            r_copy(lq, dx).start()
        else:
            mine = pl.ds(pl.multiple_of(me * piece, 128), piece)
            rown[lq, 0] = both + dec_v[pl.ds(lq * dlen, dlen), mine].astype(F32)

    def far_sums(lq):
        with scope("pair_sum"):
            for dx in range(1, nx):
                pair_sum(lq, dx)

    for lq in range(nlq):
        def own_parts(h):
            with scope("wait_res"):
                last = beyond - nlq + lq
                for side in range(2):
                    take(side, places(sides[side]) + lq, last, h)
            with scope("finish"):
                block, _ = terms(z * nlq + lq, [(side, have(side, last)) for side in range(2)])
                for i in range(h * ppairs // 2, (h + 1) * ppairs // 2):
                    t = jnp.transpose(jnp.concatenate([block(2 * i), block(2 * i + 1)], axis=0))
                    t = t.astype(BF16)
                    att[pl.ds(lq * dlen, dlen), pl.ds(2 * i * 128, 128)] = t[:HD]
                    att[pl.ds(lq * dlen, dlen), pl.ds((2 * i + 1) * 128, 128)] = t[HD:]
                if lq == 0 and h == 0:
                    pltpu.make_async_copy(ow, ow_v, ow_sem.at[0]).wait()

        for h in range(parts - 1):
            own_parts(h)
            with scope("out_part"):
                for dx in range(1, nx):
                    for k in range(2):
                        r = product(lq, seq_of(dx, (1 - c) if k == 0 else c), h, 1)
                        pacc[2 * dx - 2 + k] = r + pacc[2 * dx - 2 + k] if h else r
        own_parts(parts - 1)

        with scope("out"):
            last = parts - 1
            for dx in range(1, nx):
                theirs = product(lq, seq_of(dx, 1 - c), last, 1)
                held = product(lq, seq_of(dx, c), last, 1)
                if parts > 1:
                    theirs = theirs + pacc[2 * dx - 2]
                    held = held + pacc[2 * dx - 1]
                dsend[lq, dx] = theirs.astype(BF16)
                d_copy(lq, dx).start()
                rown[lq, dx] = held
        pl.when(c == 0)(functools.partial(far_sums, lq))

    with scope("out_near"):
        theirs = product(None, seq_of(0, 1 - c), 0, parts)
        held = product(None, seq_of(0, c), 0, parts)
        for lq in range(nlq):
            dsend[lq, 0] = theirs[lq * dlen:(lq + 1) * dlen].astype(BF16)
            d_copy(lq, 0).start()
        for lq in range(nlq):
            rown[lq, 0] = held[lq * dlen:(lq + 1) * dlen]

    @pl.when(c == 1)
    def _():
        for lq in range(nlq):
            far_sums(lq)

    with scope("near_sum"):
        for lq in range(nlq):
            pair_sum(lq, 0)

    for d in range(2):
        for o in range(beyond):
            sent = (o < places(d)) & ((o < packed) | ~at_edge(d))

            @pl.when(sent)
            def _():
                for h in range(parts):
                    result_copy(d, o, h).wait_send()
    for lq in range(nlq):
        for dx in range(nx):
            d_copy(lq, dx).wait_send()
    for lq in range(nlq):
        with scope("final"):
            total = rown[lq, 0]
            for dx in range(1, nx):
                xs = lax.rem(x + dx, nx)
                pltpu.make_async_remote_copy(
                    src_ref=xsend.at[lq, 0], dst_ref=rx.at[lq, xs], send_sem=r_send.at[lq, 0],
                    recv_sem=r_recv.at[lq, dx - 1], device_id={"seq": xs * 2 + c},
                ).wait_recv()
                total = total + rx[lq, xs].astype(F32)
            out[pl.ds(lq * dlen, dlen), :] = total.astype(BF16)
    for lq in range(nlq):
        for dx in range(1, nx):
            r_copy(lq, dx).wait_send()


def body(
    states, enc_gain, dec_states, dec_gain, query_weight, key_value_weight, out_weight, question_of
):
    nz = lax.axis_size("qset")
    n_seq = lax.axis_size("seq")
    nx = n_seq // 2
    plen, width = states.shape[2], states.shape[3]
    nlq, dlen = dec_states.shape[0], dec_states.shape[1]
    cols = query_weight.shape[1]
    rows = nlq * dlen
    piece = width // n_seq
    half = cols // 2
    nq = nlq * nz
    slots = min(3, cols // 128)
    nch = sum(CHUNKS)
    beyond = nlq * (nz - 1)
    parts = 2 if cols % 512 == 0 else 1
    cfg = (n_seq, nz, nlq, plen, dlen, width, cols)
    any_spec = pl.BlockSpec(memory_space=pl.ANY)
    dma = pltpu.SemaphoreType.DMA
    result = pl.pallas_call(
        functools.partial(kernel, cfg),
        out_shape=pltpu.VMEM((rows, piece), BF16),
        in_specs=[pl.BlockSpec(memory_space=pltpu.SMEM), any_spec, any_spec, any_spec, any_spec,
                  any_spec, any_spec, any_spec],
        out_specs=pl.BlockSpec(memory_space=pltpu.VMEM),
        scratch_shapes=[
            pltpu.VMEM((width,), BF16),
            pltpu.VMEM((width,), BF16),
            pltpu.VMEM((plen, width), BF16),
            pltpu.VMEM((rows, width), BF16),
            pltpu.VMEM((n_seq, plen, width), BF16),
            pltpu.VMEM((width, cols), BF16),
            pltpu.VMEM((slots, 2 * width, 128), BF16),
            pltpu.VMEM((1024, 128), F32),
            pltpu.VMEM((width, 2 * cols), BF16),
            pltpu.VMEM((cols, width), BF16),
            pltpu.VMEM((rows, width), BF16),
            pltpu.VMEM((n_seq, plen, 2 * cols), BF16),
            pltpu.VMEM((nq, dlen, cols), BF16),
            pltpu.VMEM((n_seq, half, 128), F32),
            pltpu.VMEM((n_seq, 8, 128), F32),
            pltpu.VMEM((2, beyond, half + 32, 128), BF16),
            pltpu.VMEM((2, beyond, half + 32, 128), BF16),
            pltpu.VMEM((2, half + 32, 128), BF16),
            pltpu.VMEM((rows, cols), BF16),
            pltpu.VMEM((nlq, nx, dlen, piece), BF16),
            pltpu.VMEM((nlq, nx, dlen, piece), BF16),
            pltpu.VMEM((nlq, nx, dlen, piece), BF16),
            pltpu.VMEM((nlq, nx, dlen, piece), BF16),
            pltpu.VMEM((nlq, nx, dlen, piece), F32),
            pltpu.VMEM((2 * cols // 128, plen, 128), F32),
            pltpu.VMEM((2 * cols // 128, plen, 128), BF16),
            pltpu.VMEM((max(8, 2 * cols // 128), 128), F32),
            pltpu.VMEM((nx - 1, plen, 2 * cols), F32),
            pltpu.VMEM((n_seq - 2, dlen, piece) if cols % 512 == 0 else (1, 8, 128), F32),
            dma((6,)), dma((slots,)), dma((1,)),
            dma((2,)), dma((2,)), dma((nx - 1, nch)), dma((nx - 1, nch)), dma((nx - 1, 2, nch)),
            dma((2, nq)), dma((nq,)), dma((2, beyond, parts)), dma((2, beyond, parts)),
            dma((nlq, nx)), dma((nlq, nx)), dma((nlq, nx - 1)), dma((nlq, nx - 1)),
        ],
        compiler_params=pltpu.CompilerParams(
            collective_id=0, has_side_effects=True, vmem_limit_bytes=63 * 1024 * 1024
        ),
        name="reader",
    )(
        question_of[:, :, 0], states.reshape(plen, width), enc_gain,
        dec_states.reshape(rows, width), dec_gain,
        query_weight, key_value_weight, out_weight,
    )
    return result.reshape(nlq, dlen, piece)


def solution(mesh):
    return jax.shard_map(
        body,
        mesh=mesh,
        in_specs=(
            P(("groups", "qset"), "seq", None, None),
            P(),
            P(("groups", "qset"), None, None),
            P(),
            P(None, "seq"),
            P(None, None, "seq"),
            P("seq", None),
            P("groups", None, None),
        ),
        out_specs=P(("groups", "qset"), None, "seq"),
        check_vma=False,
    )
```

```python
import functools
import jax
import jax.numpy as jnp
from jax import lax
from jax.experimental import pallas as pl
from jax.experimental.pallas import tpu as pltpu
from jax.sharding import PartitionSpec as P

HD = 64
EPSILON = 1e-06
DEAD = -1e30
EIGHTHS = ((4, 4), (2, 2, 2, 1, 1))
CHUNKS = tuple(len(t) for t in EIGHTHS)
KT = 1024
F32 = jnp.float32
BF16 = jnp.bfloat16
scope = jax.named_scope


def norm_rows(load, store, gain, rows):
    step = 16

    def one(i, carry):
        at = pl.multiple_of(i * step, step)
        x = load(at, step).astype(F32)
        ms = jnp.mean(x * x, axis=-1, keepdims=True)
        store(at, step, (x * lax.rsqrt(ms + EPSILON) * gain).astype(BF16))
        return carry

    lax.fori_loop(0, rows // step, one, 0, unroll=2)


def kernel(
    cfg, qo_in, states, enc_gain, dec_states, dec_gain, qw, kvw, ow, out,
    qo, eg_v, dg_v, xin, dec_v, gat, qw_v, raw, pulled, kv_v, ow_v, xn, kvs, qall, a_s, e_s,
    ps, pr, pick, att, dsend, dpart, xsend, rx, rown, s_buf, w_buf, i_buf, acc, pacc,
    local_sem, raw_sem, ow_sem, xp_send, xp_recv, xs_send, xf_send, x_recv, q_send, q_recv,
    pr_recv, d_send, d_recv, r_send, r_recv,
):
    n_seq, nz, nlq, plen, dlen, width, cols = cfg
    nx = n_seq // 2
    npairs = cols // 128
    rows = nlq * dlen
    hr = plen // 2
    srows = cols // 2
    parts = 2 if npairs % 4 == 0 else 1
    prows = srows // parts
    ppairs = npairs // parts
    beyond = nlq * (nz - 1)
    packed = min(n_seq, beyond)
    piece = width // n_seq
    me = lax.axis_index("seq")
    z = lax.axis_index("qset")
    x = me // 2
    c = lax.rem(me, 2)
    partner = x * 2 + (1 - c)
    up_ok = z < nz - 1
    down_ok = z > 0

    def seq_of(dx, core):
        return lax.rem(x + dx, nx) * 2 + core

    barrier = pltpu.get_barrier_semaphore()
    for dx in range(1, nx):
        pl.semaphore_signal(barrier, 1, device_id={"seq": seq_of(dx, c)})
    pl.semaphore_signal(barrier, 1, device_id={"seq": partner})

    @pl.when(up_ok)
    def _():
        pl.semaphore_signal(barrier, 1, device_id={"qset": z + 1})

    @pl.when(down_ok)
    def _():
        pl.semaphore_signal(barrier, 1, device_id={"qset": z - 1})

    eg_copy = pltpu.make_async_copy(enc_gain, eg_v, local_sem.at[0])
    eg_copy.start()

    def own_copy(half):
        at = pl.ds(half * hr, hr)
        return pltpu.make_async_copy(states.at[at], xin.at[at], local_sem.at[1 + half])

    own_copy(0).start()
    own_copy(1).start()
    dg_copy = pltpu.make_async_copy(dec_gain, dg_v, local_sem.at[3])
    dg_copy.start()
    dec_copy = pltpu.make_async_copy(dec_states, dec_v, local_sem.at[4])
    dec_copy.start()
    qo_copy = pltpu.make_async_copy(qo_in, qo, local_sem.at[6])
    qo_copy.start()
    qw_copy = pltpu.make_async_copy(qw, qw_v, local_sem.at[5])
    qw_copy.start()
    nblocks = cols // 128
    slots = raw.shape[0]
    kv2 = kvw.reshape(2 * width, cols)

    def raw_copy(b):
        return pltpu.make_async_copy(
            kv2.at[:, pl.ds(b * 128, 128)], raw.at[b % slots], raw_sem.at[b % slots]
        )

    def ow_copy(b):
        i, h2, k = b // 4, (b // 2) % 2, b % 2
        src = (2 * i + k) * 128 + h2 * HD
        return pltpu.make_async_copy(
            ow.at[pl.ds(src, HD)], ow_v.at[pl.ds(b * HD, HD)], ow_sem.at[0]
        )

    eg_copy.wait()
    eg = eg_v[...].astype(F32).reshape(1, width)

    def norm_own(half):
        own_copy(half).wait()

        def put(at, n, v):
            gat[me, pl.ds(half * hr + at, n), :] = v

        norm_rows(lambda at, n: xin[pl.ds(half * hr + at, n), :], put, eg, hr)

    with scope("own_norm"):
        norm_own(0)
    for b in range(min(slots, nblocks)):
        raw_copy(b).start()
    with scope("barrier"):
        pl.semaphore_wait(
            barrier, nx - 1 + 1 + up_ok.astype(jnp.int32) + down_ok.astype(jnp.int32)
        )

    def half_rows(slot, half):
        return gat.at[slot, pl.ds(pl.multiple_of(half * hr, hr), hr)]

    def to_partner(half):
        part = half_rows(me, half)
        return pltpu.make_async_remote_copy(
            src_ref=part, dst_ref=part, send_sem=xp_send.at[half], recv_sem=xp_recv.at[half],
            device_id={"seq": partner},
        )

    def from_partner(half):
        part = half_rows(partner, half)
        return pltpu.make_async_remote_copy(
            src_ref=part, dst_ref=part, send_sem=xp_send.at[half], recv_sem=xp_recv.at[half],
            device_id={"seq": partner},
        )

    def columns(k, ch):
        eighth = width // 8
        return pl.ds(sum(EIGHTHS[k][:ch]) * eighth, EIGHTHS[k][ch] * eighth)

    def x_copy(slot, half, k, ch, to, send_sem, source):
        part = gat.at[slot, pl.ds(pl.multiple_of(half * hr, hr), hr), columns(k, ch)]
        return pltpu.make_async_remote_copy(
            src_ref=part, dst_ref=part, send_sem=send_sem,
            recv_sem=x_recv.at[source, half, k * CHUNKS[0] + ch], device_id={"seq": to},
        )

    def over_x(k, dx, ch):
        return x_copy(
            x * 2 + k, c, k, ch, seq_of(dx, c), xs_send.at[dx - 1, k * CHUNKS[0] + ch],
            nx - 1 - dx,
        )

    def start_over_x(k):
        for ch in range(CHUNKS[k]):
            for dx in range(1, nx):
                over_x(k, dx, ch).start()

    def passed_on(k, dx, ch, half):
        return x_copy(
            seq_of(dx, k), half, k, ch, partner, xf_send.at[dx - 1, k * CHUNKS[0] + ch], dx - 1
        )

    def forward(k, ch):
        for dx in range(1, nx):
            passed_on(k, dx, ch, c).wait_recv()
            passed_on(k, dx, ch, c).start()

    def wait_other(k, ch):
        for dx in range(1, nx):
            passed_on(k, dx, ch, 1 - c).wait_recv()

    @pl.when(c == 0)
    def _():
        start_over_x(0)

    @pl.when(c == 1)
    def _():
        to_partner(0).start()

    with scope("own_norm"):
        norm_own(1)
    to_partner(1).start()

    @pl.when(c == 0)
    def _():
        to_partner(0).start()

    def put_xn(at, n, v):
        xn[pl.ds(at, n), :] = v

    with scope("dec_norm"):
        dg_copy.wait()
        dec_copy.wait()
        dg = dg_v[...].astype(F32).reshape(1, width)
        norm_rows(lambda at, n: dec_v[pl.ds(at, n), :], put_xn, dg, rows)

    with scope("x_start"):
        from_partner(c).wait_recv()

        @pl.when(c == 1)
        def _():
            start_over_x(0)

        start_over_x(1)

    def q_copy(up, question):
        part = qall.at[question]
        return pltpu.make_async_remote_copy(
            src_ref=part, dst_ref=part, send_sem=q_send.at[0 if up else 1, question],
            recv_sem=q_recv.at[question], device_id={"qset": z + 1 if up else z - 1},
        )

    tile = min(512, cols)
    with scope("qproj"):
        qw_copy.wait()

        def q_tile(i, carry):
            at = pl.ds(pl.multiple_of(i * tile, tile), tile)
            r = jnp.dot(xn[...], qw_v[:, at], preferred_element_type=F32).astype(BF16)
            for lq in range(nlq):
                qall[z * nlq + lq, :, at] = r[lq * dlen:(lq + 1) * dlen]
            return carry

        lax.fori_loop(0, cols // tile, q_tile, 0)
    for lq in range(nlq):
        @pl.when(up_ok)
        def _():
            q_copy(True, z * nlq + lq).start()

        @pl.when(down_ok)
        def _():
            q_copy(False, z * nlq + lq).start()

    def pass_q(j, lq):
        @pl.when((z - j >= 0) & up_ok)
        def _():
            q_copy(True, (z - j) * nlq + lq).wait_recv()
            q_copy(True, (z - j) * nlq + lq).start()

        @pl.when((z + j < nz) & down_ok)
        def _():
            q_copy(False, (z + j) * nlq + lq).wait_recv()
            q_copy(False, (z + j) * nlq + lq).start()

    step = 256

    def pull_block(b):
        raw_copy(b).wait()
        flat = raw.at[b % slots]

        def pull(i, carry):
            for u in range(4):
                s = i * 4 + u
                buf = pulled.at[pl.ds(u * step, step)]
                buf[...] = flat[pl.ds(pl.multiple_of(s * step, step), step), :].astype(F32)
                at = pl.ds(pl.multiple_of(s * (step // 2), step // 2), step // 2)
                kv_v[at, pl.ds(b * 128, 128)] = buf[pl.ds(0, step // 2, stride=2), :].astype(BF16)
                kv_v[at, pl.ds(cols + b * 128, 128)] = (
                    buf[pl.ds(1, step // 2, stride=2), :].astype(BF16)
                )
            return carry

        lax.fori_loop(0, 2 * width // step // 4, pull, 0)
        if b + slots < nblocks:
            raw_copy(b + slots).start()

    with scope("pull"):
        for b in range(nblocks):
            pull_block(b)
            if b == (nblocks + 1) // 2 and nz > 2:
                pass_q(1, 0)
    for b in range(cols // HD):
        ow_copy(b).start()

    flat_gat = gat.reshape(n_seq * plen, width)
    flat_kvs = kvs.reshape(n_seq * plen, 2 * cols)


    def project(first, count, lo, hi):
        base = pl.multiple_of(first * plen, plen)
        ktile = min(KT // count, cols)

        def kv_tile(i, carry):
            at = pl.ds(pl.multiple_of(i * ktile, ktile), ktile)
            r = jnp.dot(
                flat_gat[pl.ds(base, count * plen), :], kv_v[:, at],
                preferred_element_type=F32,
            )
            flat_kvs[pl.ds(base, count * plen), at] = r.astype(BF16)
            return carry

        lax.fori_loop(lo * cols // ktile, hi * cols // ktile, kv_tile, 0)

    with scope("fwd0"):
        forward(0, 0)
    with scope("q_fwd0"):
        if nz > 2:
            for lq in range(1, nlq):
                pass_q(1, lq)
        from_partner(1 - c).wait_recv()
    with scope("proj_own0"):
        project(x * 2, 2, 0, 1)
    with scope("q_fwd1"):
        for ch in range(1, CHUNKS[0]):
            forward(0, ch)
        if nz > 3:
            pass_q(2, 0)
    with scope("proj_own1"):
        project(x * 2, 2, 1, 2)
    with scope("fwd1"):
        forward(1, 0)
        if nz > 3:
            for lq in range(1, nlq):
                pass_q(2, lq)
        for ch in range(CHUNKS[0]):
            wait_other(0, ch)
    with scope("proj_a"):
        for dx in range(1, nx):
            project(seq_of(dx, 0), 1, 0, 2)
    with scope("q_fwd2"):
        for j in range(3, nz - 1):
            for lq in range(nlq):
                pass_q(j, lq)
    def project_part(dx, ch, starts, tile):
        p = seq_of(dx, 1)
        for start in starts:
            at = pl.ds(start, tile)
            r = jnp.dot(
                gat[p, :, columns(1, ch)], kv_v[columns(1, ch), at],
                preferred_element_type=F32,
            )
            if ch:
                r = r + acc[dx - 1, :, at]
            if ch < CHUNKS[1] - 1:
                acc[dx - 1, :, at] = r
            else:
                kvs[p, :, at] = r.astype(BF16)

    def take_part(ch):
        wait_other(1, ch)
        for dx in range(1, nx):
            project_part(dx, ch, (0, cols), cols)

    with scope("b01"):
        forward(1, 1)
        take_part(0)
        take_part(1)
    with scope("b2"):
        forward(1, 2)
        forward(1, 3)
        take_part(2)

    low = lax.broadcasted_iota(jnp.int32, (dlen, 128), 1) < HD

    def attend_all(ps_list, pairs=range(npairs)):
        units = [(u * len(pairs) + i, p, j) for u, p in enumerate(ps_list) for i, j in enumerate(pairs)]
        for n, p, j in units:
            q = qall[qo[z, p], :, pl.ds(j * 128, 128)]
            zero = jnp.zeros_like(q)
            q2 = jnp.concatenate([jnp.where(low, q, zero), jnp.where(low, zero, q)], axis=0)
            s_buf[n] = lax.dot_general(
                kvs[p, :, pl.ds(j * 128, 128)], q2, (((1,), (1,)), ((), ())),
                preferred_element_type=F32,
            )
        for n, p, j in units:
            s = s_buf[n]
            m = jnp.max(s, axis=0, keepdims=True)
            w = jnp.exp(s - m)
            l = jnp.sum(w, axis=0, keepdims=True)
            w_buf[n] = w.astype(BF16)
            i_buf[pl.ds(n, 1), :] = 1.0 / l
            e_s[p, j // ppairs, pl.ds(j % ppairs, 1), :] = m + jnp.log(l)
        for n, p, j in units:
            o = lax.dot_general(
                kvs[p, :, pl.ds(cols + j * 128, 128)], w_buf[n], (((0,), (0,)), ((), ())),
                preferred_element_type=F32,
            )
            a_s[p, pl.ds(j * HD, HD), :] = jnp.where(low, o[:HD], o[HD:]) * i_buf[n:n + 1, :]

    e_s[...] = jnp.zeros(e_s.shape, F32)
    with scope("fwd4"):
        forward(1, 4)
    with scope("wait_q"):
        qo_copy.wait()
        for question in range(nlq * nz):
            b = question // nlq

            @pl.when(((b < z) & (z == nz - 1)) | ((b > z) & (z == 0)))
            def _():
                q_copy(True, question).wait_recv()
    with scope("attend_own"):
        attend_all([x * 2, x * 2 + 1])
    with scope("b_3"):
        take_part(3)
    with scope("attend_a"):
        for dx in range(1, nx):
            attend_all([seq_of(dx, 0)])

    erows = 16

    def put_logs(ref, e, h):
        hi = e.astype(BF16).astype(F32)
        rest = e - hi
        mid = rest.astype(BF16).astype(F32)
        pieces = [t[:ppairs] for t in (hi, mid, rest - mid)]
        pieces.append(jnp.zeros((erows - 3 * ppairs, 128), F32))
        at = pl.ds(h * (prows + erows) + prows, erows)
        ref[at, :] = jnp.concatenate(pieces, axis=0).astype(BF16)

    def get_logs(ref, h):
        t = ref[pl.ds(h * (prows + erows) + prows, erows), :].astype(F32)
        e = t[:ppairs] + t[ppairs:2 * ppairs] + t[2 * ppairs:3 * ppairs]
        return jnp.concatenate([e, jnp.zeros((8 - ppairs, 128), F32)], axis=0)

    near = (2 * z >= nz).astype(jnp.int32)
    sides = (near, 1 - near)

    def question_at(d, o):
        return jnp.where(d == 0, (nz - 1 - o // nlq) * nlq, o // nlq * nlq) + o % nlq

    def packing(d):
        edge = jnp.where(d == 0, 0, nz - 1)
        rank, ranks, found = jnp.int32(0), [], []
        for o in range(beyond):
            hit = jnp.int32(0)
            for p in range(n_seq):
                hit = hit | (qo[edge, p] == question_at(d, o)).astype(jnp.int32)
            ranks.append(jnp.minimum(rank, packed - 1))
            found.append(hit)
            rank = rank + hit
        return ranks, found

    plans = [packing(d) for d in sides]

    def terms(question, sources, h):
        first = jnp.int32(0)
        second = jnp.int32(0)
        count = jnp.int32(0)
        for p in range(n_seq):
            hit = qo[z, p] == question
            first = jnp.where(hit & (count == 0), p, first)
            second = jnp.where(hit & (count == 1), p, second)
            count = count + hit.astype(jnp.int32)
        e = [jnp.where(count >= 1, e_s[first, h], DEAD), jnp.where(count >= 2, e_s[second, h], DEAD)]
        e += [jnp.where(ok, get_logs(pick.at[side], h), DEAD) for side, ok in sources]
        top = functools.reduce(jnp.maximum, e)
        w = [jnp.exp(t - top) for t in e]
        tot = functools.reduce(jnp.add, w)
        inv = 1.0 / tot
        w = [t * inv for t in w]

        def block(j):
            at = pl.ds(j * HD, HD)
            there = pl.ds(j * HD + erows * h, HD)
            values = [a_s[first, at, :], a_s[second, at, :]]
            values += [pick[side, there, :].astype(F32) for side, ok in sources]
            return functools.reduce(
                jnp.add, [t * u[j - h * ppairs:j - h * ppairs + 1, :] for t, u in zip(values, w, strict=True)]
            )

        return block, top + jnp.log(tot)

    def part_rows(h):
        return pl.ds(h * (prows + erows), prows + erows)

    def result_copy(d, n, h):
        at = part_rows(h)
        return pltpu.make_async_remote_copy(
            src_ref=ps.at[d, n, at], dst_ref=pr.at[d, n, at], send_sem=q_send.at[d, n * parts + h],
            recv_sem=pr_recv.at[d, n, h], device_id={"qset": z + 1 - 2 * d},
        )

    def at_edge(d):
        return jnp.where(d == 0, z == 0, z == nz - 1)

    def after_edge(d):
        return jnp.where(d == 0, z == 1, z == nz - 2)

    def places(d):
        return jnp.where(d == 0, nz - 1 - z, z) * nlq

    def take(side, o, packed_o, h):
        d = sides[side]
        at = part_rows(h)
        ranks, _ = plans[side]

        @pl.when(after_edge(d))
        def _():
            if packed_o < packed:
                result_copy(d, packed_o, h).wait_recv()
            value = pr[d, 0, at, :]
            for n in range(1, min(packed_o, packed - 1) + 1):
                value = jnp.where(ranks[packed_o] == n, pr[d, n, at, :], value)
            pick[side, at, :] = value

        @pl.when(~(after_edge(d) | at_edge(d)))
        def _():
            result_copy(d, o, h).wait_recv()
            pick[side, at, :] = pr[d, o, at, :]

        @pl.when(at_edge(d))
        def _():
            pick[side, at, :] = jnp.zeros((at.size, 128), BF16)

    def have(side, packed_o):
        d = sides[side]
        _, found = plans[side]
        return ~at_edge(d) & (~after_edge(d) | (found[packed_o] > 0))

    def put_slot(d, n, question, sources, h):
        block, e = terms(question, sources, h)
        for j in range(h * ppairs, (h + 1) * ppairs):
            ps[d, n, pl.ds(j * HD + erows * h, HD), :] = block(j).astype(BF16)
        put_logs(ps.at[d, n], e, h)
        result_copy(d, n, h).start()

    def nth_found(side, n):
        ranks, found = plans[side]
        question = jnp.int32(-1)
        rank = jnp.int32(0)
        for o in range(beyond):
            question = jnp.where(
                (found[o] > 0) & (rank == n), question_at(sides[side], o), question
            )
            rank = rank + found[o]
        return question

    def first_hop(side, todo):
        d = sides[side]

        @pl.when(at_edge(d))
        def _():
            for n, h in todo:
                put_slot(d, n, nth_found(side, n), [], h)

    def hop(side, o):
        d = sides[side]

        @pl.when((o < places(d)) & ~at_edge(d))
        def _():
            for h in range(parts):
                take(side, o, o, h)
                put_slot(d, o, question_at(d, o), [(side, have(side, o))], h)

    for question in range(nlq * nz):
        @pl.when(up_ok & (question // nlq <= z))
        def _():
            q_copy(True, question).wait_send()

        @pl.when(down_ok & (question // nlq >= z))
        def _():
            q_copy(False, question).wait_send()

    todo = [(n, h) for n in range(packed) for h in range(parts)]
    with scope("b3"):
        wait_other(1, CHUNKS[1] - 1)
    span = cols // parts
    for h in range(parts):
        with scope("b3"):
            for dx in range(1, nx):
                project_part(dx, CHUNKS[1] - 1, (h * span, cols + h * span), span)
        with scope("attend_b"):
            for dx in range(1, nx):
                attend_all([seq_of(dx, 1)], range(h * ppairs, (h + 1) * ppairs))
            for side in range(2):
                first_hop(side, todo[:1] if h < parts - 1 else todo[min(parts - 1, 1):])

    with scope("chain"):
        for o in range(beyond + 1):
            if o < beyond:
                hop(0, o)
            if o:
                hop(1, o - 1)

    for half in range(2):
        to_partner(half).wait_send()
    for k in range(2):
        for ch in range(CHUNKS[k]):
            for dx in range(1, nx):
                over_x(k, dx, ch).wait_send()
                passed_on(k, dx, ch, c).wait_send()


    def product(lq, dest, first, count):
        src = pl.ds(pl.multiple_of(dest * piece, piece), piece)
        heads = pl.ds(first * ppairs * 128, count * ppairs * 128)
        rows_in = pl.ds(lq * dlen, dlen) if lq is not None else pl.ds(0, rows)
        return jnp.dot(att[rows_in, heads], ow_v[heads, src], preferred_element_type=F32)

    def d_copy(lq, dx):
        return pltpu.make_async_remote_copy(
            src_ref=dsend.at[lq, dx], dst_ref=dpart.at[lq, dx], send_sem=d_send.at[lq, dx],
            recv_sem=d_recv.at[lq, dx], device_id={"seq": partner},
        )

    def r_copy(lq, dx):
        return pltpu.make_async_remote_copy(
            src_ref=xsend.at[lq, dx], dst_ref=rx.at[lq, x], send_sem=r_send.at[lq, dx - 1],
            recv_sem=r_recv.at[lq, nx - 1 - dx], device_id={"seq": seq_of(dx, c)},
        )

    def pair_sum(lq, dx):
        d_copy(lq, dx).wait_recv()
        both = rown[lq, dx] + dpart[lq, dx].astype(F32)
        if dx:
            xsend[lq, dx] = both.astype(BF16)
            r_copy(lq, dx).start()
        else:
            mine = pl.ds(pl.multiple_of(me * piece, 128), piece)
            rown[lq, 0] = both + dec_v[pl.ds(lq * dlen, dlen), mine].astype(F32)

    def far_sums(lq):
        with scope("pair_sum"):
            for dx in range(1, nx):
                pair_sum(lq, dx)

    for lq in range(nlq):
        def own_parts(h):
            with scope("wait_res"):
                last = beyond - nlq + lq
                for side in range(2):
                    take(side, places(sides[side]) + lq, last, h)
            with scope("finish"):
                block, _ = terms(z * nlq + lq, [(side, have(side, last)) for side in range(2)], h)
                for i in range(h * ppairs // 2, (h + 1) * ppairs // 2):
                    t = jnp.transpose(jnp.concatenate([block(2 * i), block(2 * i + 1)], axis=0))
                    t = t.astype(BF16)
                    att[pl.ds(lq * dlen, dlen), pl.ds(2 * i * 128, 128)] = t[:HD]
                    att[pl.ds(lq * dlen, dlen), pl.ds((2 * i + 1) * 128, 128)] = t[HD:]
                if lq == 0 and h == 0:
                    pltpu.make_async_copy(ow, ow_v, ow_sem.at[0]).wait()

        for h in range(parts - 1):
            own_parts(h)
            with scope("out_part"):
                for dx in range(1, nx):
                    for k in range(2):
                        r = product(lq, seq_of(dx, (1 - c) if k == 0 else c), h, 1)
                        pacc[2 * dx - 2 + k] = r + pacc[2 * dx - 2 + k] if h else r
        own_parts(parts - 1)

        with scope("out"):
            last = parts - 1
            for dx in range(1, nx):
                theirs = product(lq, seq_of(dx, 1 - c), last, 1)
                held = product(lq, seq_of(dx, c), last, 1)
                if parts > 1:
                    theirs = theirs + pacc[2 * dx - 2]
                    held = held + pacc[2 * dx - 1]
                dsend[lq, dx] = theirs.astype(BF16)
                d_copy(lq, dx).start()
                rown[lq, dx] = held
        far_sums(lq)

    with scope("out_near"):
        theirs = product(None, seq_of(0, 1 - c), 0, parts)
        held = product(None, seq_of(0, c), 0, parts)
        for lq in range(nlq):
            dsend[lq, 0] = theirs[lq * dlen:(lq + 1) * dlen].astype(BF16)
            d_copy(lq, 0).start()
        for lq in range(nlq):
            rown[lq, 0] = held[lq * dlen:(lq + 1) * dlen]

    with scope("near_sum"):
        for lq in range(nlq):
            pair_sum(lq, 0)

    for d in range(2):
        for o in range(beyond):
            sent = (o < places(d)) & ((o < packed) | ~at_edge(d))

            @pl.when(sent)
            def _():
                for h in range(parts):
                    result_copy(d, o, h).wait_send()
    for lq in range(nlq):
        for dx in range(nx):
            d_copy(lq, dx).wait_send()
    for lq in range(nlq):
        with scope("final"):
            total = rown[lq, 0]
            for dx in range(1, nx):
                xs = lax.rem(x + dx, nx)
                pltpu.make_async_remote_copy(
                    src_ref=xsend.at[lq, 0], dst_ref=rx.at[lq, xs], send_sem=r_send.at[lq, 0],
                    recv_sem=r_recv.at[lq, dx - 1], device_id={"seq": xs * 2 + c},
                ).wait_recv()
                total = total + rx[lq, xs].astype(F32)
            out[pl.ds(lq * dlen, dlen), :] = total.astype(BF16)
    for lq in range(nlq):
        for dx in range(1, nx):
            r_copy(lq, dx).wait_send()


def body(
    states, enc_gain, dec_states, dec_gain, query_weight, key_value_weight, out_weight, question_of
):
    nz = lax.axis_size("qset")
    n_seq = lax.axis_size("seq")
    nx = n_seq // 2
    plen, width = states.shape[2], states.shape[3]
    nlq, dlen = dec_states.shape[0], dec_states.shape[1]
    cols = query_weight.shape[1]
    rows = nlq * dlen
    piece = width // n_seq
    half = cols // 2
    nq = nlq * nz
    slots = min(3, cols // 128)
    nch = sum(CHUNKS)
    beyond = nlq * (nz - 1)
    parts = 2 if cols % 512 == 0 else 1
    cfg = (n_seq, nz, nlq, plen, dlen, width, cols)
    any_spec = pl.BlockSpec(memory_space=pl.ANY)
    dma = pltpu.SemaphoreType.DMA
    result = pl.pallas_call(
        functools.partial(kernel, cfg),
        out_shape=pltpu.VMEM((rows, piece), BF16),
        in_specs=[any_spec, any_spec, any_spec, any_spec, any_spec,
                  any_spec, any_spec, any_spec],
        out_specs=pl.BlockSpec(memory_space=pltpu.VMEM),
        scratch_shapes=[
            pltpu.SMEM((nz, n_seq), jnp.int32),
            pltpu.VMEM((width,), BF16),
            pltpu.VMEM((width,), BF16),
            pltpu.VMEM((plen, width), BF16),
            pltpu.VMEM((rows, width), BF16),
            pltpu.VMEM((n_seq, plen, width), BF16),
            pltpu.VMEM((width, cols), BF16),
            pltpu.VMEM((slots, 2 * width, 128), BF16),
            pltpu.VMEM((1024, 128), F32),
            pltpu.VMEM((width, 2 * cols), BF16),
            pltpu.VMEM((cols, width), BF16),
            pltpu.VMEM((rows, width), BF16),
            pltpu.VMEM((n_seq, plen, 2 * cols), BF16),
            pltpu.VMEM((nq, dlen, cols), BF16),
            pltpu.VMEM((n_seq, half, 128), F32),
            pltpu.VMEM((n_seq, parts, 8, 128), F32),
            pltpu.VMEM((2, beyond, half + 16 * parts, 128), BF16),
            pltpu.VMEM((2, beyond, half + 16 * parts, 128), BF16),
            pltpu.VMEM((2, half + 16 * parts, 128), BF16),
            pltpu.VMEM((rows, cols), BF16),
            pltpu.VMEM((nlq, nx, dlen, piece), BF16),
            pltpu.VMEM((nlq, nx, dlen, piece), BF16),
            pltpu.VMEM((nlq, nx, dlen, piece), BF16),
            pltpu.VMEM((nlq, nx, dlen, piece), BF16),
            pltpu.VMEM((nlq, nx, dlen, piece), F32),
            pltpu.VMEM((2 * cols // 128, plen, 128), F32),
            pltpu.VMEM((2 * cols // 128, plen, 128), BF16),
            pltpu.VMEM((max(8, 2 * cols // 128), 128), F32),
            pltpu.VMEM((nx - 1, plen, 2 * cols), F32),
            pltpu.VMEM((n_seq - 2, dlen, piece) if cols % 512 == 0 else (1, 8, 128), F32),
            dma((7,)), dma((slots,)), dma((1,)),
            dma((2,)), dma((2,)), dma((nx - 1, nch)), dma((nx - 1, nch)), dma((nx - 1, 2, nch)),
            dma((2, max(nq, beyond * parts))), dma((nq,)), dma((2, beyond, parts)),
            dma((nlq, nx)), dma((nlq, nx)), dma((nlq, nx - 1)), dma((nlq, nx - 1)),
        ],
        compiler_params=pltpu.CompilerParams(
            collective_id=0, has_side_effects=True, vmem_limit_bytes=63 * 1024 * 1024
        ),
        name="reader",
    )(
        question_of[:, :, 0], states.reshape(plen, width), enc_gain,
        dec_states.reshape(rows, width), dec_gain,
        query_weight, key_value_weight, out_weight,
    )
    return result.reshape(nlq, dlen, piece)


def solution(mesh):
    return jax.shard_map(
        body,
        mesh=mesh,
        in_specs=(
            P(("groups", "qset"), "seq", None, None),
            P(),
            P(("groups", "qset"), None, None),
            P(),
            P(None, "seq"),
            P(None, None, "seq"),
            P("seq", None),
            P("groups", None, None),
        ),
        out_specs=P(("groups", "qset"), None, "seq"),
        check_vma=False,
    )
```

```python
import functools
import jax
import jax.numpy as jnp
from jax import lax
from jax.experimental import pallas as pl
from jax.experimental.pallas import tpu as pltpu
from jax.sharding import PartitionSpec as P

HD = 64
EPSILON = 1e-06
DEAD = -1e30
EIGHTHS = ((4, 4), (2, 2, 2, 1, 1))
CHUNKS = tuple(len(t) for t in EIGHTHS)
KT = 1024
F32 = jnp.float32
BF16 = jnp.bfloat16
scope = jax.named_scope


def norm_rows(load, store, gain, rows):
    step = 16

    def one(i, carry):
        at = pl.multiple_of(i * step, step)
        x = load(at, step).astype(F32)
        ms = jnp.mean(x * x, axis=-1, keepdims=True)
        store(at, step, (x * lax.rsqrt(ms + EPSILON) * gain).astype(BF16))
        return carry

    lax.fori_loop(0, rows // step, one, 0, unroll=2)


def kernel(
    cfg, qo_in, states, enc_gain, dec_states, dec_gain, qw, kvw, ow, out,
    qo, eg_v, dg_v, xin, dec_v, gat, qw_v, raw, pulled, kv_v, ow_v, xn, kvs, qall, a_s, e_s,
    ps, pr, pick, att, dsend, dpart, xsend, rx, rown, s_buf, w_buf, i_buf, acc, pacc,
    local_sem, raw_sem, ow_sem, xp_send, xp_recv, xs_send, xf_send, x_recv, q_send, q_recv,
    pr_recv, d_send, d_recv, r_send, r_recv,
):
    n_seq, nz, nlq, plen, dlen, width, cols = cfg
    nx = n_seq // 2
    npairs = cols // 128
    rows = nlq * dlen
    hr = plen // 2
    srows = cols // 2
    parts = 2 if npairs % 4 == 0 else 1
    prows = srows // parts
    ppairs = npairs // parts
    beyond = nlq * (nz - 1)
    packed = min(n_seq, beyond)
    piece = width // n_seq
    me = lax.axis_index("seq")
    z = lax.axis_index("qset")
    x = me // 2
    c = lax.rem(me, 2)
    partner = x * 2 + (1 - c)
    up_ok = z < nz - 1
    down_ok = z > 0

    def seq_of(dx, core):
        return lax.rem(x + dx, nx) * 2 + core

    barrier = pltpu.get_barrier_semaphore()
    for dx in range(1, nx):
        pl.semaphore_signal(barrier, 1, device_id={"seq": seq_of(dx, c)})
    pl.semaphore_signal(barrier, 1, device_id={"seq": partner})

    @pl.when(up_ok)
    def _():
        pl.semaphore_signal(barrier, 1, device_id={"qset": z + 1})

    @pl.when(down_ok)
    def _():
        pl.semaphore_signal(barrier, 1, device_id={"qset": z - 1})

    eg_copy = pltpu.make_async_copy(enc_gain, eg_v, local_sem.at[0])
    eg_copy.start()

    def own_copy(half):
        at = pl.ds(half * hr, hr)
        return pltpu.make_async_copy(states.at[at], xin.at[at], local_sem.at[1 + half])

    own_copy(0).start()
    own_copy(1).start()
    dg_copy = pltpu.make_async_copy(dec_gain, dg_v, local_sem.at[3])
    dg_copy.start()
    dec_copy = pltpu.make_async_copy(dec_states, dec_v, local_sem.at[4])
    dec_copy.start()
    qo_copy = pltpu.make_async_copy(qo_in, qo, local_sem.at[6])
    qo_copy.start()
    qw_copy = pltpu.make_async_copy(qw, qw_v, local_sem.at[5])
    qw_copy.start()
    nblocks = cols // 128
    slots = raw.shape[0]
    kv2 = kvw.reshape(2 * width, cols)

    def raw_copy(b):
        return pltpu.make_async_copy(
            kv2.at[:, pl.ds(b * 128, 128)], raw.at[b % slots], raw_sem.at[b % slots]
        )

    def ow_copy(b):
        i, h2, k = b // 4, (b // 2) % 2, b % 2
        src = (2 * i + k) * 128 + h2 * HD
        return pltpu.make_async_copy(
            ow.at[pl.ds(src, HD)], ow_v.at[pl.ds(b * HD, HD)], ow_sem.at[0]
        )

    eg_copy.wait()
    eg = eg_v[...].astype(F32).reshape(1, width)

    def norm_own(half):
        own_copy(half).wait()

        def put(at, n, v):
            gat[me, pl.ds(half * hr + at, n), :] = v

        norm_rows(lambda at, n: xin[pl.ds(half * hr + at, n), :], put, eg, hr)

    with scope("own_norm"):
        norm_own(0)
    for b in range(min(slots, nblocks)):
        raw_copy(b).start()
    with scope("barrier"):
        pl.semaphore_wait(
            barrier, nx - 1 + 1 + up_ok.astype(jnp.int32) + down_ok.astype(jnp.int32)
        )

    def half_rows(slot, half):
        return gat.at[slot, pl.ds(pl.multiple_of(half * hr, hr), hr)]

    def to_partner(half):
        part = half_rows(me, half)
        return pltpu.make_async_remote_copy(
            src_ref=part, dst_ref=part, send_sem=xp_send.at[half], recv_sem=xp_recv.at[half],
            device_id={"seq": partner},
        )

    def from_partner(half):
        part = half_rows(partner, half)
        return pltpu.make_async_remote_copy(
            src_ref=part, dst_ref=part, send_sem=xp_send.at[half], recv_sem=xp_recv.at[half],
            device_id={"seq": partner},
        )

    def columns(k, ch):
        eighth = width // 8
        return pl.ds(sum(EIGHTHS[k][:ch]) * eighth, EIGHTHS[k][ch] * eighth)

    def x_copy(slot, half, k, ch, to, send_sem, source):
        part = gat.at[slot, pl.ds(pl.multiple_of(half * hr, hr), hr), columns(k, ch)]
        return pltpu.make_async_remote_copy(
            src_ref=part, dst_ref=part, send_sem=send_sem,
            recv_sem=x_recv.at[source, half, k * CHUNKS[0] + ch], device_id={"seq": to},
        )

    def over_x(k, dx, ch):
        return x_copy(
            x * 2 + k, c, k, ch, seq_of(dx, c), xs_send.at[dx - 1, k * CHUNKS[0] + ch],
            nx - 1 - dx,
        )

    def start_over_x(k):
        for ch in range(CHUNKS[k]):
            for dx in range(1, nx):
                over_x(k, dx, ch).start()

    def passed_on(k, dx, ch, half):
        return x_copy(
            seq_of(dx, k), half, k, ch, partner, xf_send.at[dx - 1, k * CHUNKS[0] + ch], dx - 1
        )

    def forward(k, ch):
        for dx in range(1, nx):
            passed_on(k, dx, ch, c).wait_recv()
            passed_on(k, dx, ch, c).start()

    def wait_other(k, ch):
        for dx in range(1, nx):
            passed_on(k, dx, ch, 1 - c).wait_recv()

    @pl.when(c == 0)
    def _():
        start_over_x(0)

    @pl.when(c == 1)
    def _():
        to_partner(0).start()

    with scope("own_norm"):
        norm_own(1)
    to_partner(1).start()

    @pl.when(c == 0)
    def _():
        to_partner(0).start()

    def put_xn(at, n, v):
        xn[pl.ds(at, n), :] = v

    with scope("dec_norm"):
        dg_copy.wait()
        dec_copy.wait()
        dg = dg_v[...].astype(F32).reshape(1, width)
        norm_rows(lambda at, n: dec_v[pl.ds(at, n), :], put_xn, dg, rows)

    with scope("x_start"):
        from_partner(c).wait_recv()

        @pl.when(c == 1)
        def _():
            start_over_x(0)

        start_over_x(1)

    def q_copy(up, question):
        part = qall.at[question]
        return pltpu.make_async_remote_copy(
            src_ref=part, dst_ref=part, send_sem=q_send.at[0 if up else 1, question],
            recv_sem=q_recv.at[question], device_id={"qset": z + 1 if up else z - 1},
        )

    tile = min(512, cols)
    with scope("qproj"):
        qw_copy.wait()

        def q_tile(i, carry):
            at = pl.ds(pl.multiple_of(i * tile, tile), tile)
            r = jnp.dot(xn[...], qw_v[:, at], preferred_element_type=F32).astype(BF16)
            for lq in range(nlq):
                qall[z * nlq + lq, :, at] = r[lq * dlen:(lq + 1) * dlen]
            return carry

        lax.fori_loop(0, cols // tile, q_tile, 0)
    for lq in range(nlq):
        @pl.when(up_ok)
        def _():
            q_copy(True, z * nlq + lq).start()

        @pl.when(down_ok)
        def _():
            q_copy(False, z * nlq + lq).start()

    def pass_q(j, lq):
        @pl.when((z - j >= 0) & up_ok)
        def _():
            q_copy(True, (z - j) * nlq + lq).wait_recv()
            q_copy(True, (z - j) * nlq + lq).start()

        @pl.when((z + j < nz) & down_ok)
        def _():
            q_copy(False, (z + j) * nlq + lq).wait_recv()
            q_copy(False, (z + j) * nlq + lq).start()

    step = 256

    def pull_block(b):
        raw_copy(b).wait()
        flat = raw.at[b % slots]

        def pull(i, carry):
            for u in range(4):
                s = i * 4 + u
                buf = pulled.at[pl.ds(u * step, step)]
                buf[...] = flat[pl.ds(pl.multiple_of(s * step, step), step), :].astype(F32)
                at = pl.ds(pl.multiple_of(s * (step // 2), step // 2), step // 2)
                kv_v[at, pl.ds(b * 128, 128)] = buf[pl.ds(0, step // 2, stride=2), :].astype(BF16)
                kv_v[at, pl.ds(cols + b * 128, 128)] = (
                    buf[pl.ds(1, step // 2, stride=2), :].astype(BF16)
                )
            return carry

        lax.fori_loop(0, 2 * width // step // 4, pull, 0)
        if b + slots < nblocks:
            raw_copy(b + slots).start()

    with scope("pull"):
        for b in range(nblocks):
            pull_block(b)
            if b == (nblocks + 1) // 2 and nz > 2:
                pass_q(1, 0)
    for b in range(cols // HD):
        ow_copy(b).start()

    flat_gat = gat.reshape(n_seq * plen, width)
    flat_kvs = kvs.reshape(n_seq * plen, 2 * cols)


    def project(first, count, lo, hi):
        base = pl.multiple_of(first * plen, plen)
        ktile = min(KT // count, cols)

        def kv_tile(i, carry):
            at = pl.ds(pl.multiple_of(i * ktile, ktile), ktile)
            r = jnp.dot(
                flat_gat[pl.ds(base, count * plen), :], kv_v[:, at],
                preferred_element_type=F32,
            )
            flat_kvs[pl.ds(base, count * plen), at] = r.astype(BF16)
            return carry

        lax.fori_loop(lo * cols // ktile, hi * cols // ktile, kv_tile, 0)

    with scope("fwd0"):
        forward(0, 0)
    with scope("q_fwd0"):
        if nz > 2:
            for lq in range(1, nlq):
                pass_q(1, lq)
        from_partner(1 - c).wait_recv()
    with scope("proj_own0"):
        project(x * 2, 2, 0, 1)
    with scope("q_fwd1"):
        for ch in range(1, CHUNKS[0]):
            forward(0, ch)
        if nz > 3:
            pass_q(2, 0)
    with scope("proj_own1"):
        project(x * 2, 2, 1, 2)
    with scope("fwd1"):
        forward(1, 0)
        if nz > 3:
            for lq in range(1, nlq):
                pass_q(2, lq)
        for ch in range(CHUNKS[0]):
            wait_other(0, ch)
    with scope("proj_a"):
        for dx in range(1, nx):
            project(seq_of(dx, 0), 1, 0, 2)
    with scope("q_fwd2"):
        for j in range(3, nz - 1):
            for lq in range(nlq):
                pass_q(j, lq)
    def project_part(dx, ch, starts, tile):
        p = seq_of(dx, 1)
        for start in starts:
            at = pl.ds(start, tile)
            r = jnp.dot(
                gat[p, :, columns(1, ch)], kv_v[columns(1, ch), at],
                preferred_element_type=F32,
            )
            if ch:
                r = r + acc[dx - 1, :, at]
            if ch < CHUNKS[1] - 1:
                acc[dx - 1, :, at] = r
            else:
                kvs[p, :, at] = r.astype(BF16)

    def take_part(ch):
        wait_other(1, ch)
        for dx in range(1, nx):
            project_part(dx, ch, (0, cols), cols)

    with scope("b01"):
        forward(1, 1)
        take_part(0)
        take_part(1)
    low = lax.broadcasted_iota(jnp.int32, (dlen, 128), 1) < HD

    def attend_all(ps_list, pairs=range(npairs)):
        units = [(u * len(pairs) + i, p, j) for u, p in enumerate(ps_list) for i, j in enumerate(pairs)]
        for n, p, j in units:
            q = qall[qo[z, p], :, pl.ds(j * 128, 128)]
            zero = jnp.zeros_like(q)
            q2 = jnp.concatenate([jnp.where(low, q, zero), jnp.where(low, zero, q)], axis=0)
            s_buf[n] = lax.dot_general(
                kvs[p, :, pl.ds(j * 128, 128)], q2, (((1,), (1,)), ((), ())),
                preferred_element_type=F32,
            )
        for n, p, j in units:
            s = s_buf[n]
            m = jnp.max(s, axis=0, keepdims=True)
            w = jnp.exp(s - m)
            l = jnp.sum(w, axis=0, keepdims=True)
            w_buf[n] = w.astype(BF16)
            i_buf[pl.ds(n, 1), :] = 1.0 / l
            e_s[p, j // ppairs, pl.ds(j % ppairs, 1), :] = m + jnp.log(l)
        for n, p, j in units:
            o = lax.dot_general(
                kvs[p, :, pl.ds(cols + j * 128, 128)], w_buf[n], (((0,), (0,)), ((), ())),
                preferred_element_type=F32,
            )
            a_s[p, pl.ds(j * HD, HD), :] = jnp.where(low, o[:HD], o[HD:]) * i_buf[n:n + 1, :]

    e_s[...] = jnp.zeros(e_s.shape, F32)
    with scope("fwd2"):
        forward(1, 2)
    with scope("wait_q"):
        qo_copy.wait()
        for question in range(nlq * nz):
            b = question // nlq

            @pl.when(((b < z) & (z == nz - 1)) | ((b > z) & (z == 0)))
            def _():
                q_copy(True, question).wait_recv()
    with scope("attend_a"):
        for dx in range(1, nx):
            attend_all([seq_of(dx, 0)])
    with scope("b2"):
        forward(1, 3)
        take_part(2)
    with scope("fwd4"):
        forward(1, 4)
    with scope("attend_own"):
        attend_all([x * 2, x * 2 + 1])
    with scope("b_3"):
        take_part(3)

    erows = 16

    def put_logs(ref, e, h):
        hi = e.astype(BF16).astype(F32)
        rest = e - hi
        mid = rest.astype(BF16).astype(F32)
        pieces = [t[:ppairs] for t in (hi, mid, rest - mid)]
        pieces.append(jnp.zeros((erows - 3 * ppairs, 128), F32))
        at = pl.ds(h * (prows + erows) + prows, erows)
        ref[at, :] = jnp.concatenate(pieces, axis=0).astype(BF16)

    def get_logs(ref, h):
        t = ref[pl.ds(h * (prows + erows) + prows, erows), :].astype(F32)
        e = t[:ppairs] + t[ppairs:2 * ppairs] + t[2 * ppairs:3 * ppairs]
        return jnp.concatenate([e, jnp.zeros((8 - ppairs, 128), F32)], axis=0)

    near = (2 * z >= nz).astype(jnp.int32)
    sides = (near, 1 - near)

    def question_at(d, o):
        return jnp.where(d == 0, (nz - 1 - o // nlq) * nlq, o // nlq * nlq) + o % nlq

    def packing(d):
        edge = jnp.where(d == 0, 0, nz - 1)
        rank, ranks, found = jnp.int32(0), [], []
        for o in range(beyond):
            hit = jnp.int32(0)
            for p in range(n_seq):
                hit = hit | (qo[edge, p] == question_at(d, o)).astype(jnp.int32)
            ranks.append(jnp.minimum(rank, packed - 1))
            found.append(hit)
            rank = rank + hit
        return ranks, found

    plans = [packing(d) for d in sides]

    def terms(question, sources, h):
        first = jnp.int32(0)
        second = jnp.int32(0)
        count = jnp.int32(0)
        for p in range(n_seq):
            hit = qo[z, p] == question
            first = jnp.where(hit & (count == 0), p, first)
            second = jnp.where(hit & (count == 1), p, second)
            count = count + hit.astype(jnp.int32)
        e = [jnp.where(count >= 1, e_s[first, h], DEAD), jnp.where(count >= 2, e_s[second, h], DEAD)]
        e += [jnp.where(ok, get_logs(pick.at[side], h), DEAD) for side, ok in sources]
        top = functools.reduce(jnp.maximum, e)
        w = [jnp.exp(t - top) for t in e]
        tot = functools.reduce(jnp.add, w)
        inv = 1.0 / tot
        w = [t * inv for t in w]

        def block(j):
            at = pl.ds(j * HD, HD)
            there = pl.ds(j * HD + erows * h, HD)
            values = [a_s[first, at, :], a_s[second, at, :]]
            values += [pick[side, there, :].astype(F32) for side, ok in sources]
            return functools.reduce(
                jnp.add, [t * u[j - h * ppairs:j - h * ppairs + 1, :] for t, u in zip(values, w, strict=True)]
            )

        return block, top + jnp.log(tot)

    def part_rows(h):
        return pl.ds(h * (prows + erows), prows + erows)

    def result_copy(d, n, h):
        at = part_rows(h)
        return pltpu.make_async_remote_copy(
            src_ref=ps.at[d, n, at], dst_ref=pr.at[d, n, at], send_sem=q_send.at[d, n * parts + h],
            recv_sem=pr_recv.at[d, n, h], device_id={"qset": z + 1 - 2 * d},
        )

    def at_edge(d):
        return jnp.where(d == 0, z == 0, z == nz - 1)

    def after_edge(d):
        return jnp.where(d == 0, z == 1, z == nz - 2)

    def places(d):
        return jnp.where(d == 0, nz - 1 - z, z) * nlq

    def take(side, o, packed_o, h):
        d = sides[side]
        at = part_rows(h)
        ranks, _ = plans[side]

        @pl.when(after_edge(d))
        def _():
            if packed_o < packed:
                result_copy(d, packed_o, h).wait_recv()
            value = pr[d, 0, at, :]
            for n in range(1, min(packed_o, packed - 1) + 1):
                value = jnp.where(ranks[packed_o] == n, pr[d, n, at, :], value)
            pick[side, at, :] = value

        @pl.when(~(after_edge(d) | at_edge(d)))
        def _():
            result_copy(d, o, h).wait_recv()
            pick[side, at, :] = pr[d, o, at, :]

        @pl.when(at_edge(d))
        def _():
            pick[side, at, :] = jnp.zeros((at.size, 128), BF16)

    def have(side, packed_o):
        d = sides[side]
        _, found = plans[side]
        return ~at_edge(d) & (~after_edge(d) | (found[packed_o] > 0))

    def put_slot(d, n, question, sources, h):
        block, e = terms(question, sources, h)
        for j in range(h * ppairs, (h + 1) * ppairs):
            ps[d, n, pl.ds(j * HD + erows * h, HD), :] = block(j).astype(BF16)
        put_logs(ps.at[d, n], e, h)
        result_copy(d, n, h).start()

    def nth_found(side, n):
        ranks, found = plans[side]
        question = jnp.int32(-1)
        rank = jnp.int32(0)
        for o in range(beyond):
            question = jnp.where(
                (found[o] > 0) & (rank == n), question_at(sides[side], o), question
            )
            rank = rank + found[o]
        return question

    def first_hop(side, todo):
        d = sides[side]

        @pl.when(at_edge(d))
        def _():
            for n, h in todo:
                put_slot(d, n, nth_found(side, n), [], h)

    def hop(side, o):
        d = sides[side]

        @pl.when((o < places(d)) & ~at_edge(d))
        def _():
            for h in range(parts):
                take(side, o, o, h)
                put_slot(d, o, question_at(d, o), [(side, have(side, o))], h)

    for question in range(nlq * nz):
        @pl.when(up_ok & (question // nlq <= z))
        def _():
            q_copy(True, question).wait_send()

        @pl.when(down_ok & (question // nlq >= z))
        def _():
            q_copy(False, question).wait_send()

    todo = [(n, h) for n in range(packed) for h in range(parts)]
    with scope("b3"):
        wait_other(1, CHUNKS[1] - 1)
    span = cols // parts
    for h in range(parts):
        with scope("b3"):
            for dx in range(1, nx):
                project_part(dx, CHUNKS[1] - 1, (h * span, cols + h * span), span)
        with scope("attend_b"):
            for dx in range(1, nx):
                attend_all([seq_of(dx, 1)], range(h * ppairs, (h + 1) * ppairs))
            for side in range(2):
                first_hop(side, todo[:1] if h < parts - 1 else todo[min(parts - 1, 1):])

    with scope("chain"):
        for o in range(beyond + 1):
            if o < beyond:
                hop(0, o)
            if o:
                hop(1, o - 1)

    for half in range(2):
        to_partner(half).wait_send()
    for k in range(2):
        for ch in range(CHUNKS[k]):
            for dx in range(1, nx):
                over_x(k, dx, ch).wait_send()
                passed_on(k, dx, ch, c).wait_send()


    def product(lq, dest, first, count):
        src = pl.ds(pl.multiple_of(dest * piece, piece), piece)
        heads = pl.ds(first * ppairs * 128, count * ppairs * 128)
        rows_in = pl.ds(lq * dlen, dlen) if lq is not None else pl.ds(0, rows)
        return jnp.dot(att[rows_in, heads], ow_v[heads, src], preferred_element_type=F32)

    def d_copy(lq, dx):
        return pltpu.make_async_remote_copy(
            src_ref=dsend.at[lq, dx], dst_ref=dpart.at[lq, dx], send_sem=d_send.at[lq, dx],
            recv_sem=d_recv.at[lq, dx], device_id={"seq": partner},
        )

    def r_copy(lq, dx):
        return pltpu.make_async_remote_copy(
            src_ref=xsend.at[lq, dx], dst_ref=rx.at[lq, x], send_sem=r_send.at[lq, dx - 1],
            recv_sem=r_recv.at[lq, nx - 1 - dx], device_id={"seq": seq_of(dx, c)},
        )

    def pair_sum(lq, dx):
        d_copy(lq, dx).wait_recv()
        both = rown[lq, dx] + dpart[lq, dx].astype(F32)
        if dx:
            xsend[lq, dx] = both.astype(BF16)
            r_copy(lq, dx).start()
        else:
            mine = pl.ds(pl.multiple_of(me * piece, 128), piece)
            rown[lq, 0] = both + dec_v[pl.ds(lq * dlen, dlen), mine].astype(F32)

    def far_sums(lq):
        with scope("pair_sum"):
            for dx in range(1, nx):
                pair_sum(lq, dx)

    for lq in range(nlq):
        def own_parts(h):
            with scope("wait_res"):
                last = beyond - nlq + lq
                for side in range(2):
                    take(side, places(sides[side]) + lq, last, h)
            with scope("finish"):
                block, _ = terms(z * nlq + lq, [(side, have(side, last)) for side in range(2)], h)
                for i in range(h * ppairs // 2, (h + 1) * ppairs // 2):
                    t = jnp.transpose(jnp.concatenate([block(2 * i), block(2 * i + 1)], axis=0))
                    t = t.astype(BF16)
                    att[pl.ds(lq * dlen, dlen), pl.ds(2 * i * 128, 128)] = t[:HD]
                    att[pl.ds(lq * dlen, dlen), pl.ds((2 * i + 1) * 128, 128)] = t[HD:]
                if lq == 0 and h == 0:
                    pltpu.make_async_copy(ow, ow_v, ow_sem.at[0]).wait()

        for h in range(parts - 1):
            own_parts(h)
            with scope("out_part"):
                for dx in range(1, nx):
                    for k in range(2):
                        r = product(lq, seq_of(dx, (1 - c) if k == 0 else c), h, 1)
                        pacc[2 * dx - 2 + k] = r + pacc[2 * dx - 2 + k] if h else r
        if lq:
            pl.when(c == 1)(functools.partial(far_sums, lq - 1))
        own_parts(parts - 1)

        with scope("out"):
            last = parts - 1
            for dx in range(1, nx):
                theirs = product(lq, seq_of(dx, 1 - c), last, 1)
                held = product(lq, seq_of(dx, c), last, 1)
                if parts > 1:
                    theirs = theirs + pacc[2 * dx - 2]
                    held = held + pacc[2 * dx - 1]
                dsend[lq, dx] = theirs.astype(BF16)
                d_copy(lq, dx).start()
                rown[lq, dx] = held
        if lq < nlq - 1:
            pl.when(c == 0)(functools.partial(far_sums, lq))
        else:
            far_sums(lq)

    with scope("out_near"):
        theirs = product(None, seq_of(0, 1 - c), 0, parts)
        held = product(None, seq_of(0, c), 0, parts)
        for lq in range(nlq):
            dsend[lq, 0] = theirs[lq * dlen:(lq + 1) * dlen].astype(BF16)
            d_copy(lq, 0).start()
        for lq in range(nlq):
            rown[lq, 0] = held[lq * dlen:(lq + 1) * dlen]

    with scope("near_sum"):
        for lq in range(nlq):
            pair_sum(lq, 0)

    for d in range(2):
        for o in range(beyond):
            sent = (o < places(d)) & ((o < packed) | ~at_edge(d))

            @pl.when(sent)
            def _():
                for h in range(parts):
                    result_copy(d, o, h).wait_send()
    for lq in range(nlq):
        for dx in range(nx):
            d_copy(lq, dx).wait_send()
    for lq in range(nlq):
        with scope("final"):
            total = rown[lq, 0]
            for dx in range(1, nx):
                xs = lax.rem(x + dx, nx)
                pltpu.make_async_remote_copy(
                    src_ref=xsend.at[lq, 0], dst_ref=rx.at[lq, xs], send_sem=r_send.at[lq, 0],
                    recv_sem=r_recv.at[lq, dx - 1], device_id={"seq": xs * 2 + c},
                ).wait_recv()
                total = total + rx[lq, xs].astype(F32)
            out[pl.ds(lq * dlen, dlen), :] = total.astype(BF16)
    for lq in range(nlq):
        for dx in range(1, nx):
            r_copy(lq, dx).wait_send()


def body(
    states, enc_gain, dec_states, dec_gain, query_weight, key_value_weight, out_weight, question_of
):
    nz = lax.axis_size("qset")
    n_seq = lax.axis_size("seq")
    nx = n_seq // 2
    plen, width = states.shape[2], states.shape[3]
    nlq, dlen = dec_states.shape[0], dec_states.shape[1]
    cols = query_weight.shape[1]
    rows = nlq * dlen
    piece = width // n_seq
    half = cols // 2
    nq = nlq * nz
    slots = min(3, cols // 128)
    nch = sum(CHUNKS)
    beyond = nlq * (nz - 1)
    parts = 2 if cols % 512 == 0 else 1
    cfg = (n_seq, nz, nlq, plen, dlen, width, cols)
    any_spec = pl.BlockSpec(memory_space=pl.ANY)
    dma = pltpu.SemaphoreType.DMA
    result = pl.pallas_call(
        functools.partial(kernel, cfg),
        out_shape=pltpu.VMEM((rows, piece), BF16),
        in_specs=[any_spec, any_spec, any_spec, any_spec, any_spec,
                  any_spec, any_spec, any_spec],
        out_specs=pl.BlockSpec(memory_space=pltpu.VMEM),
        scratch_shapes=[
            pltpu.SMEM((nz, n_seq), jnp.int32),
            pltpu.VMEM((width,), BF16),
            pltpu.VMEM((width,), BF16),
            pltpu.VMEM((plen, width), BF16),
            pltpu.VMEM((rows, width), BF16),
            pltpu.VMEM((n_seq, plen, width), BF16),
            pltpu.VMEM((width, cols), BF16),
            pltpu.VMEM((slots, 2 * width, 128), BF16),
            pltpu.VMEM((1024, 128), F32),
            pltpu.VMEM((width, 2 * cols), BF16),
            pltpu.VMEM((cols, width), BF16),
            pltpu.VMEM((rows, width), BF16),
            pltpu.VMEM((n_seq, plen, 2 * cols), BF16),
            pltpu.VMEM((nq, dlen, cols), BF16),
            pltpu.VMEM((n_seq, half, 128), F32),
            pltpu.VMEM((n_seq, parts, 8, 128), F32),
            pltpu.VMEM((2, beyond, half + 16 * parts, 128), BF16),
            pltpu.VMEM((2, beyond, half + 16 * parts, 128), BF16),
            pltpu.VMEM((2, half + 16 * parts, 128), BF16),
            pltpu.VMEM((rows, cols), BF16),
            pltpu.VMEM((nlq, nx, dlen, piece), BF16),
            pltpu.VMEM((nlq, nx, dlen, piece), BF16),
            pltpu.VMEM((nlq, nx, dlen, piece), BF16),
            pltpu.VMEM((nlq, nx, dlen, piece), BF16),
            pltpu.VMEM((nlq, nx, dlen, piece), F32),
            pltpu.VMEM((2 * cols // 128, plen, 128), F32),
            pltpu.VMEM((2 * cols // 128, plen, 128), BF16),
            pltpu.VMEM((max(8, 2 * cols // 128), 128), F32),
            pltpu.VMEM((nx - 1, plen, 2 * cols), F32),
            pltpu.VMEM((n_seq - 2, dlen, piece) if cols % 512 == 0 else (1, 8, 128), F32),
            dma((7,)), dma((slots,)), dma((1,)),
            dma((2,)), dma((2,)), dma((nx - 1, nch)), dma((nx - 1, nch)), dma((nx - 1, 2, nch)),
            dma((2, max(nq, beyond * parts))), dma((nq,)), dma((2, beyond, parts)),
            dma((nlq, nx)), dma((nlq, nx)), dma((nlq, nx - 1)), dma((nlq, nx - 1)),
        ],
        compiler_params=pltpu.CompilerParams(
            collective_id=0, has_side_effects=True, vmem_limit_bytes=63 * 1024 * 1024
        ),
        name="reader",
    )(
        question_of[:, :, 0], states.reshape(plen, width), enc_gain,
        dec_states.reshape(rows, width), dec_gain,
        query_weight, key_value_weight, out_weight,
    )
    return result.reshape(nlq, dlen, piece)


def solution(mesh):
    return jax.shard_map(
        body,
        mesh=mesh,
        in_specs=(
            P(("groups", "qset"), "seq", None, None),
            P(),
            P(("groups", "qset"), None, None),
            P(),
            P(None, "seq"),
            P(None, None, "seq"),
            P("seq", None),
            P("groups", None, None),
        ),
        out_specs=P(("groups", "qset"), None, "seq"),
        check_vma=False,
    )
```
